32 devices in a mesh: lat: 4 (over z), lon: 8 (over y, x, core).
Axes of the slice: x: 2, y: 2, z: 4, core: 2. Of those that a mesh axis runs over, the one named last changes fastest.
Arguments:
- latent: bfloat16 [48, 576, 512], P('lat', 'lon'), may hold values from -1000 to 1000
- w_qkv: bfloat16 [512, 1536], replicated, may hold values from -1 to 1
- w_proj: bfloat16 [512, 512], replicated, may hold values from -0.25 to 0.25
- w_fc1: bfloat16 [512, 2048], replicated, may hold values from -0.25 to 0.25
- w_fc2: bfloat16 [2048, 512], replicated, may hold values from -0.125 to 0.125
- w_head: bfloat16 [512, 1024], replicated, may hold values from -4 to 4
- target_bins: int32 [48, 576, 4], P('lat', 'lon'), may hold values from 0 to 255
- land_mask: int32 [48, 576], P('lat', 'lon'), may hold values 0 or 1
Outputs:
- grad_latent: bfloat16 [48, 576, 512], P('lat', 'lon')
- grad_qkv: float32 [512, 1536], P(('lat', 'lon'))
- grad_proj: float32 [512, 512], P(('lat', 'lon'))
- grad_fc1: float32 [512, 2048], P(('lat', 'lon'))
- grad_fc2: float32 [2048, 512], P(('lat', 'lon'))
- grad_head: float32 [512, 1024], P(('lat', 'lon'))
The draws below stay inside these ranges and needn't reach their ends.
All inputs are finite; a program needn't handle non-finite values. No bound on the sum of `land_mask` on one device may be relied on, other than what follows from the above.
Results may differ from the reference program's by a relative error of at most 0.015.
Values may be sent and summed in bfloat16 or wider, within the bound.
A program may use at most 128 MiB of HBM per device.

```python
import math
import jax
import jax.numpy as jnp
from jax import lax

D = 512
HEADS = 8
FF = 2048
BINS = 256
VARS = 4
WIN_LAT = 6
WIN_LON = 12
HEAD_DIM = 64
NLAT = 48
NLON = 576


def draw_latent(key, part):
    key_noise, key_scale, key_other = jax.random.split(jax.random.fold_in(key, 1), 3)
    noise_vals = jax.random.normal(key_noise, (NLAT, NLON, D), jnp.float32)
    token_scale = jnp.exp(jax.random.uniform(key_scale, (NLAT, NLON, 1), jnp.float32, 0.0, math.log(10.0)))
    feature_scale = jnp.exp(jax.random.uniform(key_other, (D,), jnp.float32, 0.0, math.log(10.0)))
    values_out = token_scale * feature_scale * noise_vals
    return jnp.clip(values_out, -1000.0, 1000.0).astype(jnp.bfloat16)


def draw_w_qkv(key, part):
    base_vals = jax.random.normal(jax.random.fold_in(key, 2), (D, 3 * D), jnp.float32) / math.sqrt(D)
    return jnp.clip(base_vals, -1.0, 1.0).astype(jnp.bfloat16)


def draw_w_head(key, part):
    base_vals = jax.random.normal(jax.random.fold_in(key, 4), (D, VARS * BINS), jnp.float32) * (3.0 / math.sqrt(D))
    return jnp.clip(base_vals, -4.0, 4.0).astype(jnp.bfloat16)


def plant(entries, stream_key, least, largest):
    dims = entries.shape
    index_at = [jax.random.randint(jax.random.fold_in(stream_key, axis), (), 0, dims[axis]) for axis in range(len(dims))]
    entries = entries.at[tuple(index_at)].set(least)
    longest = dims.index(max(dims))
    index_at[longest] = (index_at[longest] + 1) % dims[longest]
    return entries.at[tuple(index_at)].set(largest)


def noise(stream_key, dims, spread, most, kind=jnp.bfloat16):
    return jnp.clip(spread * jax.random.normal(stream_key, dims, jnp.float32), -most, most).astype(kind)


def setup_inputs(seed: int = 0) -> dict:
    key_of = jax.random.split(jax.random.key(seed), 9)
    latent = draw_latent(jax.random.fold_in(key_of[8], 71), 0)
    w_qkv = draw_w_qkv(jax.random.fold_in(key_of[8], 71), 0)
    w_proj = noise(key_of[2], (D, D), D ** -0.5, 0.25)
    w_fc1 = noise(key_of[3], (D, FF), D ** -0.5, 0.25)
    w_fc2 = noise(key_of[4], (FF, D), FF ** -0.5, 0.125)
    w_head = draw_w_head(jax.random.fold_in(key_of[8], 71), 0)
    target_bins = plant(jax.random.randint(key_of[6], (NLAT, NLON, VARS), 0, BINS), jax.random.fold_in(key_of[6], 1), 0, BINS - 1).astype(jnp.int32)
    land_mask = plant((jax.random.randint(key_of[7], (NLAT, NLON), 0, 4) < 3).astype(jnp.int32), jax.random.fold_in(key_of[7], 1), 0, 1)
    return dict(latent=latent, w_qkv=w_qkv, w_proj=w_proj, w_fc1=w_fc1, w_fc2=w_fc2, w_head=w_head, target_bins=target_bins, land_mask=land_mask)


eps = 1e-05
smear = 0.75
masked = -1e+30

def normalize(values_in):
    centre = lax.optimization_barrier(jnp.mean(values_in, -1, keepdims=True))
    offset = values_in - centre
    inverse = lax.rsqrt(lax.optimization_barrier(jnp.mean(offset * offset, -1, keepdims=True)) + eps)
    return (offset * inverse, inverse)

def norm_back(scaled, inverse, upstream):
    return inverse * (upstream - lax.optimization_barrier(jnp.mean(upstream, -1, keepdims=True)) - scaled * lax.optimization_barrier(jnp.mean(upstream * scaled, -1, keepdims=True)))

def gelu_parts(pre_act):
    normal_cdf = 0.5 * (1.0 + jax.scipy.special.erf(pre_act / math.sqrt(2.0)))
    density = jnp.exp(-0.5 * pre_act * pre_act) / math.sqrt(2.0 * math.pi)
    return (pre_act * normal_cdf, normal_cdf + pre_act * density)

def mixing(form, left, right):
    return jnp.einsum(form, left.astype(jnp.float32), right.astype(jnp.float32))

def to_windows(block):
    row_count, col_count, feat_count = block.shape
    shaped = block.reshape(row_count // WIN_LAT, WIN_LAT, col_count // WIN_LON, WIN_LON, feat_count)
    return shaped.transpose(0, 2, 1, 3, 4).reshape(-1, WIN_LAT * WIN_LON, feat_count)

def from_windows(packed, row_count, col_count):
    feat_count = packed.shape[-1]
    shaped = packed.reshape(row_count // WIN_LAT, col_count // WIN_LON, WIN_LAT, WIN_LON, feat_count)
    return shaped.transpose(0, 2, 1, 3, 4).reshape(row_count, col_count, feat_count)

def window_setup(qkv_all, row_labels):
    row_count, col_count, _ = qkv_all.shape
    packed = to_windows(qkv_all)
    heads_view = packed.reshape(packed.shape[0], packed.shape[1], 3, HEADS, HEAD_DIM)
    window_tags = to_windows(jnp.broadcast_to(row_labels[:, None, None], (row_count, col_count, 1)))[:, :, 0]
    allowed = window_tags[:, :, None] == window_tags[:, None, :]
    scores = mixing('wqhd,wkhd->whqk', heads_view[:, :, 0], heads_view[:, :, 1]) * HEAD_DIM ** (-0.5)
    scores = jnp.where(allowed[:, None], scores, masked)
    highest = lax.optimization_barrier(jnp.max(scores, -1, keepdims=True))
    exponent = jnp.exp(scores - highest)
    return (heads_view, exponent / lax.optimization_barrier(jnp.sum(exponent, -1, keepdims=True)))

def window_forward(heads_view, attn_probs, row_count, col_count):
    context = mixing('whqk,wkhd->wqhd', attn_probs.astype(jnp.bfloat16), heads_view[:, :, 2]).astype(jnp.bfloat16)
    return from_windows(context.reshape(context.shape[0], context.shape[1], -1), row_count, col_count)

def window_backward(heads_view, attn_probs, d_context, row_count, col_count):
    probs_low = attn_probs.astype(jnp.bfloat16)
    upstream = to_windows(d_context).reshape(heads_view.shape[0], heads_view.shape[1], HEADS, HEAD_DIM)
    d_probs = mixing('wqhd,wkhd->whqk', upstream, heads_view[:, :, 2])
    d_value = mixing('whqk,wqhd->wkhd', probs_low, upstream)
    d_scores = attn_probs * (d_probs - lax.optimization_barrier(jnp.sum(d_probs * attn_probs, -1, keepdims=True))) * HEAD_DIM ** (-0.5)
    d_scores = d_scores.astype(jnp.bfloat16)
    d_query = mixing('whqk,wkhd->wqhd', d_scores, heads_view[:, :, 1])
    d_key = mixing('whqk,wqhd->wkhd', d_scores, heads_view[:, :, 0])
    joined = jnp.stack([d_query, d_key, d_value], 2).astype(jnp.bfloat16)
    return from_windows(joined.reshape(joined.shape[0], joined.shape[1], -1), row_count, col_count)

def hl_target(bin_index):
    bin_edges = jnp.arange(BINS + 1, dtype=jnp.int32).astype(jnp.float32)
    centre = bin_index.astype(jnp.float32)[..., None] + 0.5
    cumulative = 0.5 * jax.scipy.special.erf((bin_edges - centre) / (smear * math.sqrt(2.0)))
    return (cumulative[..., 1:] - cumulative[..., :-1]) / (cumulative[..., -1:] - cumulative[..., :1])

def head_grad(normed3, w_head, target_bins, land_mask):
    logits = jnp.dot(normed3, w_head, preferred_element_type=jnp.float32).reshape(-1, VARS, BINS)
    highest = lax.optimization_barrier(jnp.max(logits, -1, keepdims=True))
    exponent = jnp.exp(logits - highest)
    bin_probs = exponent / lax.optimization_barrier(jnp.sum(exponent, -1, keepdims=True))
    weight_tok = land_mask.reshape(-1).astype(jnp.float32)[:, None, None] / VARS
    d_logits = weight_tok * (bin_probs - hl_target(target_bins.reshape(-1, VARS)))
    return d_logits.astype(jnp.bfloat16).reshape(-1, VARS * BINS)

def reference(latent, w_qkv, w_proj, w_fc1, w_fc2, w_head, target_bins, land_mask):
    half_rows = WIN_LAT // 2
    half_cols = WIN_LON // 2
    feat_width = latent.shape[-1]
    residual_in = latent.astype(jnp.float32)
    scaled1, inverse1 = normalize(residual_in)
    normed1 = scaled1.astype(jnp.bfloat16)
    shifted = jnp.roll(normed1, (-half_rows, -half_cols), (0, 1))
    qkv_all = jnp.dot(shifted.reshape(-1, feat_width), w_qkv, preferred_element_type=jnp.float32).astype(jnp.bfloat16)
    qkv_rows = qkv_all.reshape(NLAT // WIN_LAT, WIN_LAT, NLON, 3 * feat_width)
    row_labels = (jnp.arange(NLAT, dtype=jnp.int32) + half_rows >= NLAT).astype(jnp.int32)
    label_rows = row_labels.reshape(NLAT // WIN_LAT, WIN_LAT)

    def context_rows(packed_in):
        heads_view, attn_probs = window_setup(packed_in[0], packed_in[1])
        return window_forward(heads_view, attn_probs, WIN_LAT, NLON)
    context = lax.map(context_rows, (qkv_rows, label_rows)).reshape(-1, feat_width)
    attended = jnp.dot(context, w_proj, preferred_element_type=jnp.float32).astype(jnp.bfloat16)
    attended = jnp.roll(attended.reshape(NLAT, NLON, feat_width), (half_rows, half_cols), (0, 1))
    attended = lax.optimization_barrier(attended)
    residual = residual_in + attended.astype(jnp.float32)
    scaled2, inverse2 = normalize(residual)
    normed2 = scaled2.astype(jnp.bfloat16).reshape(-1, feat_width)
    pre_act = jnp.dot(normed2, w_fc1, preferred_element_type=jnp.float32)
    activated, gelu_slope = gelu_parts(pre_act)
    activated = activated.astype(jnp.bfloat16)
    block_out = residual + jnp.dot(activated, w_fc2, preferred_element_type=jnp.float32).reshape(NLAT, NLON, feat_width)
    scaled3, inverse3 = normalize(block_out)
    normed3 = scaled3.astype(jnp.bfloat16).reshape(-1, feat_width)
    d_logits = head_grad(normed3, w_head, target_bins, land_mask)
    grad_head = jnp.dot(normed3.T, d_logits, preferred_element_type=jnp.float32)
    d_out = norm_back(scaled3, inverse3, jnp.dot(d_logits, w_head.T, preferred_element_type=jnp.float32).reshape(NLAT, NLON, feat_width))
    d_outb = d_out.astype(jnp.bfloat16).reshape(-1, feat_width)
    grad_fc2 = jnp.dot(activated.T, d_outb, preferred_element_type=jnp.float32)
    d_pre = (jnp.dot(d_outb, w_fc2.T, preferred_element_type=jnp.float32) * gelu_slope).astype(jnp.bfloat16)
    grad_fc1 = jnp.dot(normed2.T, d_pre, preferred_element_type=jnp.float32)
    d_resid = d_out + norm_back(scaled2, inverse2, jnp.dot(d_pre, w_fc1.T, preferred_element_type=jnp.float32).reshape(NLAT, NLON, feat_width))
    d_attended = jnp.roll(d_resid.astype(jnp.bfloat16), (-half_rows, -half_cols), (0, 1)).reshape(-1, feat_width)
    grad_proj = jnp.dot(context.T, d_attended, preferred_element_type=jnp.float32)
    d_context = jnp.dot(d_attended, w_proj.T, preferred_element_type=jnp.float32).astype(jnp.bfloat16)
    d_context_rows = d_context.reshape(NLAT // WIN_LAT, WIN_LAT, NLON, feat_width)

    def gradient_rows(packed_in):
        heads_view, attn_probs = window_setup(packed_in[0], packed_in[1])
        return window_backward(heads_view, attn_probs, packed_in[2], WIN_LAT, NLON)
    d_qkv = lax.map(gradient_rows, (qkv_rows, label_rows, d_context_rows)).reshape(-1, 3 * feat_width)
    grad_qkv = jnp.dot(shifted.reshape(-1, feat_width).T, d_qkv, preferred_element_type=jnp.float32)
    d_shifted = jnp.dot(d_qkv, w_qkv.T, preferred_element_type=jnp.float32).astype(jnp.bfloat16)
    d_shifted = jnp.roll(d_shifted.reshape(NLAT, NLON, feat_width), (half_rows, half_cols), (0, 1))
    d_shifted = lax.optimization_barrier(d_shifted)
    grad_latent = (d_resid + norm_back(scaled1, inverse1, d_shifted.astype(jnp.float32))).astype(jnp.bfloat16)
    return (grad_latent, grad_qkv, grad_proj, grad_fc1, grad_fc2, grad_head)
```

```python
import functools
import math
import types

import jax
import jax.numpy as jnp
from jax import lax
from jax.experimental import pallas as pl
from jax.experimental.pallas import tpu as pltpu
from jax.sharding import PartitionSpec as P

HEADS = 8
BINS = 256
VARS = 4
WIN_LAT = 6
WIN_LON = 12
HEAD_DIM = 64
TOKENS = WIN_LAT * WIN_LON
HALF_ROWS = WIN_LAT // 2
HALF_COLS = WIN_LON // 2
EDGE = 8
LANES = 128
TILE = 256

eps = 1e-05
smear = 0.75
masked = -1e30
SOFTMAX_SCALE = HEAD_DIM ** (-0.5) / math.log(2.0)
GROUP = 2
F32 = jnp.float32
BF16 = jnp.bfloat16


def dot_nn(left, right):
    return lax.dot_general(left, right, (((1,), (0,)), ((), ())), preferred_element_type=F32)


def dot_nt(left, right):
    return lax.dot_general(left, right, (((1,), (1,)), ((), ())), preferred_element_type=F32)


def normalize(values_in):
    centre = jnp.mean(values_in, -1, keepdims=True)
    offset = values_in - centre
    inverse = lax.rsqrt(jnp.mean(offset * offset, -1, keepdims=True) + eps)
    return (offset * inverse, inverse)


def norm_back(scaled, inverse, upstream):
    return inverse * (
        upstream
        - jnp.mean(upstream, -1, keepdims=True)
        - scaled * jnp.mean(upstream * scaled, -1, keepdims=True)
    )


def loop(count, body):
    def step(place, carry):
        body(place)
        return carry

    lax.fori_loop(0, count, step, 0)


def rows_at(place, size):
    return pl.ds(pl.multiple_of(place * size, math.gcd(size, 16)), size)


def cols_at(place, size=TILE):
    return pl.ds(pl.multiple_of(place * size, size), size)


def row_block(count, most):
    best = 16
    for size in range(16, most + 1, 16):
        if count % size == 0:
            best = size
    return best


def pair_stack(block):
    lane = lax.broadcasted_iota(jnp.int32, block.shape, 1)
    low = lane < HEAD_DIM
    return jnp.concatenate([jnp.where(low, block, 0.0), jnp.where(low, 0.0, block)], 0).astype(BF16)


def pair_merge(stacked):
    top, bottom = stacked[:TOKENS], stacked[TOKENS:]
    lane = lax.broadcasted_iota(jnp.int32, top.shape, 1)
    return jnp.where(lane < HEAD_DIM, top, bottom)


def cut_windows(main, east, south, corner, strip, wins):
    row_count, col_count = main.shape[0], main.shape[1]
    own_rows = row_count - HALF_ROWS
    across, pitch = col_count // WIN_LON, col_count + EDGE
    for row in range(row_count):
        if row < own_rows:
            body, edge = main[row + HALF_ROWS], east[row + HALF_ROWS]
        else:
            body, edge = south[row - own_rows], corner[row - own_rows]
        strip[row * pitch : row * pitch + col_count] = body.astype(F32)
        strip[row * pitch + col_count : (row + 1) * pitch] = edge.astype(F32)[:EDGE]
    for row in range(row_count):
        for col in range(across):
            start = ((row // WIN_LAT) * across + col) * TOKENS + (row % WIN_LAT) * WIN_LON
            first = row * pitch + HALF_COLS + col * WIN_LON
            wins[start : start + WIN_LON] = strip[first : first + WIN_LON]


def join_windows(wins, strip, row_count, col_count):
    across, pitch = col_count // WIN_LON, col_count + EDGE
    for row in range(row_count):
        for col in range(across):
            start = ((row // WIN_LAT) * across + col) * TOKENS + (row % WIN_LAT) * WIN_LON
            first = row * pitch + HALF_COLS + col * WIN_LON
            strip[first : first + WIN_LON] = wins[start : start + WIN_LON]


def fill_table(upper, lower):
    scale = smear * math.sqrt(2.0)

    def mass_below(edge, centre):
        return 0.5 * lax.erf((edge - centre) / scale)

    def part(place):
        base = place * 64
        centre = (base + lax.broadcasted_iota(jnp.int32, (64, BINS), 0)).astype(F32) + 0.5
        edge = lax.broadcasted_iota(jnp.int32, (64, BINS), 1).astype(F32)
        whole = mass_below(float(BINS), centre) - mass_below(0.0, centre)
        table = (mass_below(edge + 1.0, centre) - mass_below(edge, centre)) / whole
        high = table.astype(BF16)
        upper[pl.ds(pl.multiple_of(base, 64), 64)] = high
        lower[pl.ds(pl.multiple_of(base, 64), 64)] = (table - high.astype(F32)).astype(BF16)

    loop(BINS // 64, part)


class Summed:
    def __init__(self, link, refs, out):
        self.link, self.out = link, out
        self.whole, self.pair, self.first, self.second, self.plane, self.slots = refs[:6]
        self.semaphores = refs[6:]
        self.half = self.plane.shape[-1] // 2
        self.copies = []

    def copy(self, place, source, target, where):
        send, recv = self.semaphores
        made = pltpu.make_async_remote_copy(
            src_ref=source, dst_ref=target, send_sem=send.at[place], recv_sem=recv.at[place],
            device_id=where, device_id_type=pl.DeviceIdType.MESH,
        )
        made.start()
        self.copies.append(made)

    def start(self):
        link = self.link
        self.copy(0, self.whole.at[:, :, :, 1 - link.core], self.pair, link.over(1))

    def spread(self):
        link, half = self.link, self.half
        self.copies[0].wait_recv()

        def add(row):
            self.pair[row] = self.pair[row] + self.whole[row, :, :, link.core]

        loop(self.pair.shape[0], add)
        self.copy(1, self.pair.at[:, :, 1 - link.x, :, :half], self.first, link.over(2))
        self.copy(2, self.pair.at[:, 1 - link.y, :, :, half:], self.second, link.over(4))

    def cross(self):
        link, half = self.link, self.half
        self.copies[1].wait_recv()

        def add_first(row):
            self.first[row] = self.first[row] + self.pair[row, :, link.x, :, :half]

        loop(self.pair.shape[0], add_first)
        self.copy(3, self.first.at[:, 1 - link.y], self.plane.at[:, :, :half], link.over(4))
        self.copies[2].wait_recv()

        def add_second(row):
            self.second[row] = self.second[row] + self.pair[row, link.y, :, :, half:]

        loop(self.pair.shape[0], add_second)
        self.copy(4, self.second.at[:, 1 - link.x], self.plane.at[:, :, half:], link.over(2))

    def deal(self):
        link, half = self.link, self.half
        self.copies[3].wait_recv()
        self.copies[4].wait_recv()

        def add(row):
            self.plane[row, :, :half] = self.plane[row, :, :half] + self.first[row, link.y]
            self.plane[row, :, half:] = self.plane[row, :, half:] + self.second[row, link.x]

        loop(self.plane.shape[0], add)
        for step in range(1, link.lats):
            there = lax.rem(link.lat + step, link.lats)
            self.copy(4 + step, self.plane.at[there], self.slots.at[step - 1], (there, link.lon))

    def finish(self):
        link = self.link
        total = self.plane[link.lat].astype(F32)
        for step in range(1, link.lats):
            self.copies[4 + step].wait_recv()
            total = total + self.slots[step - 1].astype(F32)
        self.out[...] = total

    def drain(self):
        for made in self.copies:
            made.wait_send()


class Link:
    def __init__(self, lats, lons):
        self.lats, self.lons = lats, lons
        self.lat, self.lon = lax.axis_index("lat"), lax.axis_index("lon")
        self.core = lax.rem(self.lon, 2)
        self.x = lax.rem(self.lon // 2, 2)
        self.y = lax.rem(self.lon // 4, 2)

    def over(self, step):
        bit = lax.rem(self.lon // step, 2)
        return (self.lat, self.lon + step - 2 * step * bit)

    def at(self, north, west):
        return (
            lax.rem(self.lat + self.lats + north, self.lats),
            lax.rem(self.lon + self.lons + west, self.lons),
        )

    def greet(self):
        barrier = pltpu.get_barrier_semaphore()
        peers = [self.over(1), self.over(2), self.over(4)]
        peers += [self.at(step, 0) for step in range(1, self.lats)]
        peers += [self.at(0, 1), self.at(0, -1), self.at(1, 1), self.at(-1, -1)]
        for peer in peers:
            pl.semaphore_signal(barrier, inc=1, device_id=peer, device_id_type=pl.DeviceIdType.MESH)
        pl.semaphore_wait(barrier, len(peers))


def step_kernel(row_total, lats, lons, linked, names, *refs):
    r = types.SimpleNamespace(**dict(zip(names, refs)))
    main, marks = r.main, r.marks
    w_qkv, w_proj, w_fc1, w_fc2, w_head = r.w_qkv, r.w_proj, r.w_fc1, r.w_fc2, r.w_head
    latent, marks_win, normed1, qkv, probs = r.latent, r.marks_win, r.normed1, r.qkv, r.probs
    context, residual, normed2, activated = r.context, r.residual, r.normed2, r.activated
    slope, block_out, normed3, d_logits = r.slope, r.block_out, r.normed3, r.d_logits
    d_out, flipped, upper, lower = r.d_out, r.flipped, r.upper, r.lower
    strip = context
    row_count, col_count, width = main.shape
    total = row_count * col_count
    windows = total // TOKENS
    across = col_count // WIN_LON
    pairs = width // LANES
    block = row_block(total, 288)
    blocks = total // block
    wide = row_block(total, 448)
    wide_blocks = total // wide
    ff = w_fc1.shape[1]
    pitch = col_count + EDGE

    edge_copies = []
    if linked:
        link = Link(lats, lons)
        link.greet()

        def edge_copy(source, target, where):
            place = len(edge_copies)
            made = pltpu.make_async_remote_copy(
                src_ref=source, dst_ref=target, send_sem=r.edge_send.at[place],
                recv_sem=r.edge_recv.at[place], device_id=where,
                device_id_type=pl.DeviceIdType.MESH,
            )
            made.start()
            edge_copies.append(made)

        edges = (r.east, r.south, r.corner), (r.marks_east, r.marks_south, r.marks_corner)
        for grid, (east, south, corner) in zip((main, marks), edges):
            edge_copy(grid.at[:, : 2 * EDGE], east, link.at(0, -1))
            edge_copy(grid.at[:HALF_ROWS], south, link.at(-1, 0))
            edge_copy(grid.at[:HALF_ROWS, : 2 * EDGE], corner, link.at(-1, -1))
        sums = {
            name: Summed(link, [getattr(r, f"{name}{part}") for part in range(8)], getattr(r, "g_" + name))
            for name in GRADS
        }

    def advance(name, stage):
        if linked:
            stage(sums[name])

    def put(name, cols, value):
        if linked:
            whole = sums[name].whole
            whole[:, :, :, :, :, cols] = value.astype(BF16).reshape(*whole.shape[:5], TILE)
        else:
            getattr(r, "g_" + name)[:, cols] = value.astype(BF16)

    fill_table(upper, lower)
    for made in edge_copies:
        made.wait_recv()
    cut_windows(main, r.east, r.south, r.corner, strip, latent)
    cut_windows(marks, r.marks_east, r.marks_south, r.marks_corner, r.marks_strip, marks_win)

    def flip(source):
        for col in range(width // LANES):
            part = source[:total, col * LANES : (col + 1) * LANES]
            flipped[col * LANES : (col + 1) * LANES, :] = part.astype(BF16).T

    def weight_grad(name, right):
        def tile(place):
            put(name, cols_at(place), dot_nn(flipped[...], right[:, cols_at(place)].astype(BF16)))

        loop(right.shape[1] // TILE, tile)

    def first_norm(place):
        rows = rows_at(place, block)
        normed1[rows] = normalize(latent[rows])[0].astype(BF16)

    loop(blocks, first_norm)

    def project(place):
        qkv[:, cols_at(place)] = dot_nn(normed1[...], w_qkv[:, cols_at(place)])

    loop(3 * width // TILE, project)

    device_row = lax.axis_index("lat") * row_count + HALF_ROWS

    def units(place):
        return [(place * GROUP + part, pair) for part in range(GROUP) for pair in range(pairs)]

    def attend(place):
        place_q = lax.broadcasted_iota(jnp.int32, (TOKENS, TOKENS), 0)
        place_k = lax.broadcasted_iota(jnp.int32, (TOKENS, TOKENS), 1)
        bias = {}
        for part in range(GROUP):
            window = place * GROUP + part
            limit = (row_total - device_row - (window // across) * WIN_LAT) * WIN_LON
            alike = jnp.where((place_q >= limit) == (place_k >= limit), 0.0, masked)
            bias[part] = jnp.concatenate([alike, alike], 0)
        scores = []
        for index, (window, pair) in enumerate(units(place)):
            rows, start = rows_at(window, TOKENS), pair * LANES
            query = pair_stack(qkv[rows, start : start + LANES])
            key = qkv[rows, width + start : width + start + LANES].astype(BF16)
            scores.append(dot_nt(query, key) + bias[index // pairs])
        for score, (window, pair) in zip(scores, units(place)):
            exponent = jnp.exp2((score - jnp.max(score, -1, keepdims=True)) * SOFTMAX_SCALE)
            probs[window * pairs + pair] = exponent * (1.0 / jnp.sum(exponent, -1, keepdims=True))
        for window, pair in units(place):
            rows, start = rows_at(window, TOKENS), pair * LANES
            value = qkv[rows, 2 * width + start : 2 * width + start + LANES].astype(BF16)
            chance = probs[window * pairs + pair].astype(BF16)
            context[rows, start : start + LANES] = pair_merge(dot_nn(chance, value))

    loop(windows // GROUP, attend)

    def after_attention(place):
        rows = rows_at(place, block)
        attended = dot_nn(context[rows].astype(BF16), w_proj[...]).astype(BF16)
        summed = latent[rows] + attended.astype(F32)
        residual[rows] = summed
        normed2[rows] = normalize(summed)[0].astype(BF16)

    loop(blocks, after_attention)

    def widen(place):
        cols = cols_at(place // wide_blocks)
        rows = rows_at(place % wide_blocks, wide)
        pre_act = dot_nn(normed2[rows], w_fc1[:, cols])
        cdf = 0.5 * (1.0 + lax.erf(pre_act * (1.0 / math.sqrt(2.0))))
        density = jnp.exp2(pre_act * pre_act * (-0.5 / math.log(2.0))) * (1.0 / math.sqrt(2.0 * math.pi))
        activated[rows, cols] = (pre_act * cdf).astype(BF16)
        slope[rows, cols] = cdf + pre_act * density

    loop(wide_blocks * (ff // TILE), widen)

    def narrow(place):
        rows = rows_at(place, block)
        out = residual[rows] + dot_nn(activated[rows], w_fc2[...])
        block_out[rows] = out
        normed3[rows] = normalize(out)[0].astype(BF16)

    loop(blocks, narrow)

    def head(place):
        rows = rows_at(place, block)
        mark = marks_win[rows]
        weight_tok = mark[:, VARS : VARS + 1] / VARS
        bins = lax.broadcasted_iota(jnp.int32, (block, BINS), 1).astype(F32)
        for var in range(VARS):
            logits = dot_nn(normed3[rows], w_head[:, var * BINS : (var + 1) * BINS])
            exponent = jnp.exp(logits - jnp.max(logits, -1, keepdims=True))
            chance = exponent * (1.0 / jnp.sum(exponent, -1, keepdims=True))
            picked = jnp.where(mark[:, var : var + 1] == bins, 1.0, 0.0).astype(BF16)
            target = dot_nn(picked, upper[...]) + dot_nn(picked, lower[...])
            d_logits[rows, var * BINS : (var + 1) * BINS] = (weight_tok * (chance - target)).astype(BF16)

    loop(blocks, head)

    flip(normed3)
    weight_grad("head", d_logits)
    advance("head", Summed.start)
    d_outb = normed3

    def head_back(place):
        rows = rows_at(place, block)
        scaled, inverse = normalize(block_out[rows])
        back = norm_back(scaled, inverse, dot_nt(d_logits[rows], w_head[...]))
        d_out[rows] = back
        d_outb[rows] = back.astype(BF16)

    loop(blocks, head_back)
    advance("head", Summed.spread)

    fc2_rows = 4 * ff // (lats * lons) if linked else TILE

    def grad_narrow(place):
        grad = dot_nn(activated[:, cols_at(place, fc2_rows)].T, d_outb[...]).astype(BF16)
        if linked:
            whole = sums["fc2"].whole
            whole[place // 2, place % 2] = grad.reshape(*whole.shape[2:])
        else:
            r.g_fc2[rows_at(place, fc2_rows)] = grad

    loop(ff // fc2_rows, grad_narrow)
    advance("fc2", Summed.start)
    advance("head", Summed.cross)

    d_pre = slope

    def widen_back(place):
        cols = cols_at(place)
        back = dot_nt(d_outb[...], w_fc2[rows_at(place, TILE)])
        d_pre[:, cols] = back * slope[:, cols]

    loop(ff // TILE, widen_back)
    advance("fc2", Summed.spread)
    advance("head", Summed.deal)

    flip(normed2)
    weight_grad("fc1", d_pre)
    advance("fc1", Summed.start)

    d_attended = d_outb
    d_resid = d_out

    def residual_back(place):
        rows = rows_at(place, block)
        scaled, inverse = normalize(residual[rows])
        back = d_out[rows] + norm_back(scaled, inverse, dot_nt(d_pre[rows].astype(BF16), w_fc1[...]))
        d_resid[rows] = back
        d_attended[rows] = back.astype(BF16)

    loop(blocks, residual_back)
    advance("fc2", Summed.cross)
    advance("fc1", Summed.spread)

    flip(context)
    weight_grad("proj", d_attended)
    advance("proj", Summed.start)
    advance("head", Summed.finish)

    d_context = context

    def context_back(place):
        rows = rows_at(place, block)
        d_context[rows] = dot_nt(d_attended[rows], w_proj[...])

    loop(blocks, context_back)
    advance("fc2", Summed.deal)
    advance("proj", Summed.spread)

    def attend_back(place):
        d_probs = []
        for window, pair in units(place):
            rows, start = rows_at(window, TOKENS), pair * LANES
            upstream = pair_stack(d_context[rows, start : start + LANES])
            at_v = slice(2 * width + start, 2 * width + start + LANES)
            d_probs.append(dot_nt(upstream, qkv[rows, at_v].astype(BF16)))
            chance_t = probs[window * pairs + pair].T.astype(BF16)
            qkv[rows, at_v] = dot_nn(chance_t, upstream)
        for d_prob, (window, pair) in zip(d_probs, units(place)):
            rows, start = rows_at(window, TOKENS), pair * LANES
            at_q, at_k = slice(start, start + LANES), slice(width + start, width + start + LANES)
            query = pair_stack(qkv[rows, at_q])
            key = qkv[rows, at_k].astype(BF16)
            chance = probs[window * pairs + pair]
            inner = jnp.sum(d_prob * chance, -1, keepdims=True)
            d_scores = chance * (d_prob - inner) * HEAD_DIM ** (-0.5)
            qkv[rows, at_q] = pair_merge(dot_nn(d_scores.astype(BF16), key))
            qkv[rows, at_k] = dot_nn(d_scores.T.astype(BF16), query)

    def some_windows(first, last):
        loop(last - first, lambda window: attend_back(first + window))

    groups = windows // GROUP
    some_windows(0, groups // 3)
    advance("fc1", Summed.cross)
    some_windows(groups // 3, 2 * groups // 3)
    advance("proj", Summed.cross)
    advance("fc2", Summed.finish)
    advance("fc1", Summed.deal)
    advance("proj", Summed.deal)
    some_windows(2 * groups // 3, groups)

    flip(normed1)
    weight_grad("qkv", qkv)
    advance("qkv", Summed.start)
    advance("fc1", Summed.finish)
    advance("proj", Summed.finish)
    advance("qkv", Summed.spread)

    def latent_back(place):
        rows = rows_at(place, block)
        d_shifted = dot_nt(qkv[rows].astype(BF16), w_qkv[...]).astype(BF16)
        scaled, inverse = normalize(latent[rows])
        block_out[rows] = d_resid[rows] + norm_back(scaled, inverse, d_shifted.astype(F32))

    loop(blocks, latent_back)
    join_windows(block_out, strip, row_count, col_count)
    if not linked:
        for row in range(row_count):
            r.g_main[row] = strip[row * pitch : row * pitch + col_count].astype(BF16)
            r.g_edge[row] = strip[row * pitch + col_count : (row + 1) * pitch].astype(BF16)
        return

    own_rows = row_count - HALF_ROWS
    pad = jnp.zeros((EDGE, width), F32)
    for row in range(row_count):
        edge = jnp.concatenate([strip[row * pitch + col_count : (row + 1) * pitch], pad], 0)
        if row < own_rows:
            r.to_east[row] = edge.astype(BF16)
        else:
            r.to_corner[row - own_rows] = edge.astype(BF16)
            r.to_south[row - own_rows] = strip[row * pitch : row * pitch + col_count].astype(BF16)
    first_back = len(edge_copies)
    edge_copy(r.to_east, r.from_west, link.at(0, 1))
    edge_copy(r.to_south, r.from_north, link.at(1, 0))
    edge_copy(r.to_corner, r.from_corner, link.at(1, 1))
    advance("qkv", Summed.cross)

    ours = lax.broadcasted_iota(jnp.int32, (EDGE, width), 0) >= HALF_COLS

    def put_row(row, body, edge):
        head = jnp.where(ours, body[:EDGE], edge[:EDGE])
        r.g_main[row] = jnp.concatenate([head, body[EDGE:]], 0).astype(BF16)

    advance("qkv", Summed.deal)
    for made in edge_copies[first_back:]:
        made.wait_recv()
    for row in range(own_rows):
        body = strip[row * pitch : row * pitch + col_count]
        put_row(row + HALF_ROWS, body, r.from_west[row].astype(F32))
    for row in range(HALF_ROWS):
        put_row(row, r.from_north[row].astype(F32), r.from_corner[row].astype(F32))
    advance("qkv", Summed.finish)
    for made in edge_copies:
        made.wait_send()
    for name in GRADS:
        sums[name].drain()


GRADS = ("qkv", "proj", "fc1", "fc2", "head")


def device_step(latent, edges, marks, marks_edges, weights, lats, lons, linked):
    row_count, col_count, width = latent.shape
    total = row_count * col_count
    windows = total // TOKENS
    ff = weights[2].shape[1]
    lanes = marks.shape[-1]
    padded = row_count * (col_count + EDGE)
    w_qkv, w_proj, w_fc1, w_fc2, w_head = weights
    ins = dict(main=latent, marks=marks)
    if not linked:
        ins |= dict(zip(("east", "south", "corner"), edges))
        ins |= dict(zip(("marks_east", "marks_south", "marks_corner"), marks_edges))
    ins |= dict(w_qkv=w_qkv, w_proj=w_proj, w_fc1=w_fc1, w_fc2=w_fc2, w_head=w_head)
    outs = dict(g_main=jax.ShapeDtypeStruct((row_count, col_count, width), BF16))
    if not linked:
        outs |= dict(g_edge=jax.ShapeDtypeStruct((row_count, EDGE, width), BF16))
    for name, weight in zip(GRADS, weights):
        rows = weight.shape[0] // (lats * lons if linked else 1)
        outs["g_" + name] = jax.ShapeDtypeStruct((rows, weight.shape[1]), F32 if linked else BF16)
    scratch = dict(
        marks_strip=pltpu.VMEM((padded, lanes), F32),
        latent=pltpu.VMEM((total, width), F32),
        marks_win=pltpu.VMEM((total, lanes), F32),
        normed1=pltpu.VMEM((total, width), BF16),
        qkv=pltpu.VMEM((total, 3 * width), F32),
        probs=pltpu.VMEM((windows * (width // LANES), 2 * TOKENS, TOKENS), F32),
        context=pltpu.VMEM((padded, width), F32),
        residual=pltpu.VMEM((total, width), F32),
        normed2=pltpu.VMEM((total, width), BF16),
        activated=pltpu.VMEM((total, ff), BF16),
        slope=pltpu.VMEM((total, ff), F32),
        block_out=pltpu.VMEM((total, width), F32),
        normed3=pltpu.VMEM((total, width), BF16),
        d_logits=pltpu.VMEM((total, VARS * BINS), BF16),
        d_out=pltpu.VMEM((total, width), F32),
        flipped=pltpu.VMEM((width, total), BF16),
        upper=pltpu.VMEM((BINS, BINS), BF16),
        lower=pltpu.VMEM((BINS, BINS), BF16),
    )
    if linked:
        own_rows = row_count - HALF_ROWS
        wide, high, both = (row_count, 2 * EDGE), (HALF_ROWS, col_count), (HALF_ROWS, 2 * EDGE)
        own = (own_rows, 2 * EDGE)
        scratch |= dict(
            east=pltpu.VMEM((*wide, width), BF16),
            south=pltpu.VMEM((*high, width), BF16),
            corner=pltpu.VMEM((*both, width), BF16),
            marks_east=pltpu.VMEM((*wide, lanes), BF16),
            marks_south=pltpu.VMEM((*high, lanes), BF16),
            marks_corner=pltpu.VMEM((*both, lanes), BF16),
            to_east=pltpu.VMEM((*own, width), BF16),
            to_south=pltpu.VMEM((*high, width), BF16),
            to_corner=pltpu.VMEM((*both, width), BF16),
            from_west=pltpu.VMEM((*own, width), BF16),
            from_north=pltpu.VMEM((*high, width), BF16),
            from_corner=pltpu.VMEM((*both, width), BF16),
            edge_send=pltpu.SemaphoreType.DMA((9,)),
            edge_recv=pltpu.SemaphoreType.DMA((9,)),
        )
        for name, weight in zip(GRADS, weights):
            rows, cols = weight.shape[0] // (lats * lons), weight.shape[1]
            stages = [
                pltpu.VMEM((lats, 2, 2, 2, rows, cols), BF16),
                pltpu.VMEM((lats, 2, 2, rows, cols), BF16),
                pltpu.VMEM((lats, 2, rows, cols // 2), BF16),
                pltpu.VMEM((lats, 2, rows, cols // 2), BF16),
                pltpu.VMEM((lats, rows, cols), BF16),
                pltpu.VMEM((lats - 1, rows, cols), BF16),
                pltpu.SemaphoreType.DMA((4 + lats,)),
                pltpu.SemaphoreType.DMA((4 + lats,)),
            ]
            scratch |= {f"{name}{place}": stage for place, stage in enumerate(stages)}
    vmem = pl.BlockSpec(memory_space=pltpu.VMEM)
    names = [*ins, *outs, *scratch]
    done = pl.pallas_call(
        functools.partial(step_kernel, row_count * lats, lats, lons, linked, names),
        in_specs=[vmem] * len(ins),
        out_specs=[vmem] * len(outs),
        out_shape=list(outs.values()),
        scratch_shapes=list(scratch.values()),
        compiler_params=pltpu.CompilerParams(
            vmem_limit_bytes=67043328,
            **(dict(collective_id=0, has_side_effects=True) if linked else {}),
        ),
        cost_estimate=pl.CostEstimate(flops=20_000_000_000, bytes_accessed=20_000_000, transcendentals=0),
        name="device_step",
    )(*ins.values())
    return done


def moved(value, axis, steps):
    count = lax.axis_size(axis)
    pairs = [(source, (source + steps) % count) for source in range(count)]
    return lax.ppermute(value, axis, pairs)


def edges_ahead(block):
    east = moved(block[:, :EDGE], "lon", -1)
    south = moved(block[:HALF_ROWS], "lat", -1)
    return east, south, moved(east[:HALF_ROWS], "lat", -1)


def roll_behind(body, edge):
    own_rows = body.shape[0] - HALF_ROWS
    west = moved(edge, "lon", 1)[:, :HALF_COLS]
    whole = jnp.concatenate([west, body[:, HALF_COLS:]], 1)
    north = moved(whole[own_rows:], "lat", 1)
    return jnp.concatenate([north, whole[:own_rows]], 0)


def scatter_over(value, axis):
    return lax.psum_scatter(value, axis, scatter_dimension=0, tiled=True)


def local(latent, w_qkv, w_proj, w_fc1, w_fc2, w_head, target_bins, land_mask):
    width = latent.shape[2]
    lats, lons = lax.axis_size("lat"), lax.axis_size("lon")
    devices = lats * lons
    linked = lons == 8 and lats > 2 and width % (16 * devices) == 0
    marks = jnp.concatenate([target_bins, land_mask[:, :, None]], 2).astype(BF16)
    marks = jnp.pad(marks, ((0, 0), (0, 0), (0, LANES - marks.shape[2])))
    weights = (w_qkv, w_proj, w_fc1, w_fc2, w_head)
    if linked:
        return tuple(device_step(latent, (), marks, (), weights, lats, lons, True))
    body, edge, *grads = device_step(
        latent, edges_ahead(latent), marks, edges_ahead(marks), weights, lats, lons, False
    )
    grad_latent = roll_behind(body, edge)

    def to_columns(grad):
        deep = grad.shape[0] // width
        parts = grad.reshape(devices, deep, width // devices, -1)
        return [parts[:, part].reshape(width, -1) for part in range(deep)]

    columns = [to_columns(grad) for grad in grads]
    joined = jnp.concatenate([part for group in columns for part in group], 1)
    summed = scatter_over(scatter_over(joined, "lat"), "lon").astype(F32)
    outs, start = [], 0
    for grad, group in zip(grads, columns):
        size = grad.shape[1]
        pieces = [summed[:, start + part * size : start + (part + 1) * size] for part in range(len(group))]
        outs.append(jnp.concatenate(pieces, 0))
        start += size * len(group)
    return (grad_latent, *outs)


def solution(mesh):
    grid = P("lat", "lon", None)
    spread = P(("lat", "lon"), None)
    return jax.shard_map(
        local,
        mesh=mesh,
        in_specs=(grid, P(), P(), P(), P(), P(), grid, P("lat", "lon")),
        out_specs=(grid, spread, spread, spread, spread, spread),
        check_vma=False,
    )
```

```python
import functools
import math
import types

import jax
import jax.numpy as jnp
from jax import lax
from jax.experimental import pallas as pl
from jax.experimental.pallas import tpu as pltpu
from jax.sharding import PartitionSpec as P

HEADS = 8
BINS = 256
VARS = 4
WIN_LAT = 6
WIN_LON = 12
HEAD_DIM = 64
TOKENS = WIN_LAT * WIN_LON
HALF_ROWS = WIN_LAT // 2
HALF_COLS = WIN_LON // 2
EDGE = 8
LANES = 128
TILE = 256

eps = 1e-05
smear = 0.75
masked = -1e30
SOFTMAX_SCALE = HEAD_DIM ** (-0.5) / math.log(2.0)

F32 = jnp.float32
BF16 = jnp.bfloat16


def dot_nn(left, right):
    return lax.dot_general(left, right, (((1,), (0,)), ((), ())), preferred_element_type=F32)


def dot_nt(left, right):
    return lax.dot_general(left, right, (((1,), (1,)), ((), ())), preferred_element_type=F32)


def normalize(values_in):
    centre = jnp.mean(values_in, -1, keepdims=True)
    offset = values_in - centre
    inverse = lax.rsqrt(jnp.mean(offset * offset, -1, keepdims=True) + eps)
    return (offset * inverse, inverse)


def norm_back(scaled, inverse, upstream):
    return inverse * (
        upstream
        - jnp.mean(upstream, -1, keepdims=True)
        - scaled * jnp.mean(upstream * scaled, -1, keepdims=True)
    )


def loop(count, body):
    def step(place, carry):
        body(place)
        return carry

    lax.fori_loop(0, count, step, 0)


def rows_at(place, size):
    return pl.ds(pl.multiple_of(place * size, math.gcd(size, 16)), size)


def cols_at(place, size=TILE):
    return pl.ds(pl.multiple_of(place * size, size), size)


def row_block(count, most):
    best = 16
    for size in range(16, most + 1, 16):
        if count % size == 0:
            best = size
    return best


def pair_stack(block):
    lane = lax.broadcasted_iota(jnp.int32, block.shape, 1)
    low = lane < HEAD_DIM
    return jnp.concatenate([jnp.where(low, block, 0.0), jnp.where(low, 0.0, block)], 0).astype(BF16)


def pair_merge(stacked):
    top, bottom = stacked[:TOKENS], stacked[TOKENS:]
    lane = lax.broadcasted_iota(jnp.int32, top.shape, 1)
    return jnp.where(lane < HEAD_DIM, top, bottom)


def cut_windows(part, main, east, south, corner, strip, wins):
    row_count, col_count = main.shape[0], main.shape[1]
    own_rows = row_count - HALF_ROWS
    across, pitch = col_count // WIN_LON, col_count + EDGE
    for row in range(part * WIN_LAT, (part + 1) * WIN_LAT):
        if row < own_rows:
            body, edge = main[row + HALF_ROWS], east[row + HALF_ROWS]
        else:
            body, edge = south[row - own_rows], corner[row - own_rows]
        strip[row * pitch : row * pitch + col_count] = body.astype(F32)
        strip[row * pitch + col_count : (row + 1) * pitch] = edge.astype(F32)[:EDGE]
    for row in range(part * WIN_LAT, (part + 1) * WIN_LAT):
        for col in range(across):
            start = (part * across + col) * TOKENS + (row % WIN_LAT) * WIN_LON
            first = row * pitch + HALF_COLS + col * WIN_LON
            wins[start : start + WIN_LON] = strip[first : first + WIN_LON]


def join_windows(wins, strip, row_count, col_count):
    across, pitch = col_count // WIN_LON, col_count + EDGE
    for row in range(row_count):
        for col in range(across):
            start = ((row // WIN_LAT) * across + col) * TOKENS + (row % WIN_LAT) * WIN_LON
            first = row * pitch + HALF_COLS + col * WIN_LON
            strip[first : first + WIN_LON] = wins[start : start + WIN_LON]


def fill_table(upper, lower):
    scale = smear * math.sqrt(2.0)

    def mass_below(edge, centre):
        return 0.5 * lax.erf((edge - centre) / scale)

    def part(place):
        base = place * 64
        centre = (base + lax.broadcasted_iota(jnp.int32, (64, BINS), 0)).astype(F32) + 0.5
        edge = lax.broadcasted_iota(jnp.int32, (64, BINS), 1).astype(F32)
        whole = mass_below(float(BINS), centre) - mass_below(0.0, centre)
        table = (mass_below(edge + 1.0, centre) - mass_below(edge, centre)) / whole
        high = table.astype(BF16)
        upper[pl.ds(pl.multiple_of(base, 64), 64)] = high
        lower[pl.ds(pl.multiple_of(base, 64), 64)] = (table - high.astype(F32)).astype(BF16)

    loop(BINS // 64, part)


class Summed:
    def __init__(self, link, refs, out):
        self.link, self.out = link, out
        self.whole, self.pair, self.first, self.second, self.plane, self.slots = refs[:6]
        self.semaphores = refs[6:]
        self.half = self.plane.shape[-1] // 2
        self.copies = []

    def copy(self, place, source, target, where):
        send, recv = self.semaphores
        made = pltpu.make_async_remote_copy(
            src_ref=source, dst_ref=target, send_sem=send.at[place], recv_sem=recv.at[place],
            device_id=where, device_id_type=pl.DeviceIdType.MESH,
        )
        made.start()
        self.copies.append(made)

    def start(self):
        link = self.link
        self.copy(0, self.whole.at[:, :, :, 1 - link.core], self.pair, link.over(1))

    def spread(self):
        link, half = self.link, self.half
        self.copies[0].wait_recv()

        def add(row):
            self.pair[row] = self.pair[row] + self.whole[row, :, :, link.core]

        loop(self.pair.shape[0], add)
        self.copy(1, self.pair.at[:, :, 1 - link.x, :, :half], self.first, link.over(2))
        self.copy(2, self.pair.at[:, 1 - link.y, :, :, half:], self.second, link.over(4))

    def cross(self):
        link, half = self.link, self.half
        self.copies[1].wait_recv()

        def add_first(row):
            self.first[row] = self.first[row] + self.pair[row, :, link.x, :, :half]

        loop(self.pair.shape[0], add_first)
        self.copy(3, self.first.at[:, 1 - link.y], self.plane.at[:, :, :half], link.over(4))
        self.copies[2].wait_recv()

        def add_second(row):
            self.second[row] = self.second[row] + self.pair[row, link.y, :, :, half:]

        loop(self.pair.shape[0], add_second)
        self.copy(4, self.second.at[:, 1 - link.x], self.plane.at[:, :, half:], link.over(2))

    def deal(self):
        link, half = self.link, self.half
        self.copies[3].wait_recv()
        self.copies[4].wait_recv()

        def add(row):
            self.plane[row, :, :half] = self.plane[row, :, :half] + self.first[row, link.y]
            self.plane[row, :, half:] = self.plane[row, :, half:] + self.second[row, link.x]

        loop(self.plane.shape[0], add)
        for step in range(1, link.lats):
            there = lax.rem(link.lat + step, link.lats)
            self.copy(4 + step, self.plane.at[there], self.slots.at[step - 1], (there, link.lon))

    def finish(self):
        link = self.link
        total = self.plane[link.lat].astype(F32)
        for step in range(1, link.lats):
            self.copies[4 + step].wait_recv()
            total = total + self.slots[step - 1].astype(F32)
        self.out[...] = total

    def drain(self):
        for made in self.copies:
            made.wait_send()


class Link:
    def __init__(self, lats, lons):
        self.lats, self.lons = lats, lons
        self.lat, self.lon = lax.axis_index("lat"), lax.axis_index("lon")
        self.core = lax.rem(self.lon, 2)
        self.x = lax.rem(self.lon // 2, 2)
        self.y = lax.rem(self.lon // 4, 2)

    def over(self, step):
        bit = lax.rem(self.lon // step, 2)
        return (self.lat, self.lon + step - 2 * step * bit)

    def at(self, north, west):
        return (
            lax.rem(self.lat + self.lats + north, self.lats),
            lax.rem(self.lon + self.lons + west, self.lons),
        )

    def greet(self):
        barrier = pltpu.get_barrier_semaphore()
        peers = [self.over(1), self.over(2), self.over(4)]
        peers += [self.at(step, 0) for step in range(1, self.lats)]
        peers += [self.at(0, 1), self.at(0, -1), self.at(1, 1), self.at(-1, -1)]
        for peer in peers:
            pl.semaphore_signal(barrier, inc=1, device_id=peer, device_id_type=pl.DeviceIdType.MESH)
        pl.semaphore_wait(barrier, len(peers))


def step_kernel(row_total, lats, lons, linked, names, *refs):
    r = types.SimpleNamespace(**dict(zip(names, refs)))
    main, marks = r.main, r.marks
    w_qkv, w_proj, w_fc1, w_fc2, w_head = (getattr(r, f"held{place}") for place in range(5))
    arrivals = [
        pltpu.make_async_copy(getattr(r, f"weight{place}"), getattr(r, f"held{place}"), r.weight_sem.at[place])
        for place in range(5)
    ]
    for place in (0, 1, 2, 3, 4):
        arrivals[place].start()
    latent, marks_win, normed1, qkv, probs = r.latent, r.marks_win, r.normed1, r.qkv, r.probs
    context, residual, normed2, activated = r.context, r.residual, r.normed2, r.activated
    slope, block_out, normed3, d_logits = r.slope, r.block_out, r.normed3, r.d_logits
    d_out, flipped, upper, lower = r.d_out, r.flipped, r.upper, r.lower
    strip = context
    strip_in = r.residual
    row_count, col_count, width = main.shape
    total = row_count * col_count
    windows = total // TOKENS
    across = col_count // WIN_LON
    pairs = width // LANES
    group = 2 - across % 2
    block = row_block(total, 288)
    blocks = total // block
    wide = row_block(total, 448)
    wide_blocks = total // wide
    ff = w_fc1.shape[1]
    pitch = col_count + EDGE

    edge_copies = []
    if linked:
        link = Link(lats, lons)
        link.greet()

        def edge_copy(source, target, where):
            place = len(edge_copies)
            made = pltpu.make_async_remote_copy(
                src_ref=source, dst_ref=target, send_sem=r.edge_send.at[place],
                recv_sem=r.edge_recv.at[place], device_id=where,
                device_id_type=pl.DeviceIdType.MESH,
            )
            made.start()
            edge_copies.append(made)

        edge_copy(main.at[:, : 2 * EDGE], r.east, link.at(0, -1))
        edge_copy(main.at[:HALF_ROWS], r.south, link.at(-1, 0))
        edge_copy(main.at[:HALF_ROWS, : 2 * EDGE], r.corner, link.at(-1, -1))
        sums = {
            name: Summed(link, [getattr(r, f"{name}{part}") for part in range(8)], getattr(r, "g_" + name))
            for name in GRADS
        }

    def advance(name, stage):
        if linked:
            stage(sums[name])

    def put(name, cols, value):
        if linked:
            whole = sums[name].whole
            whole[:, :, :, :, :, cols] = value.astype(BF16).reshape(*whole.shape[:5], TILE)
        else:
            getattr(r, "g_" + name)[:, cols] = value.astype(BF16)

    def arrived(*places):
        for place in places:
            if linked:
                edge_copies[place].wait_recv()

    def fill_marks(row):
        pad = jnp.zeros((8 - VARS - 1, col_count), F32)
        bins, land = r.target[row].astype(F32), r.land[row : row + 1].astype(F32)
        marks[row, :, :8] = jnp.concatenate([bins, land, pad], 0).T

    for row in range(row_count):
        fill_marks(row)
    if linked:
        edge_copy(marks.at[:, :EDGE], r.marks_east, link.at(0, -1))
        edge_copy(marks.at[:HALF_ROWS], r.marks_south, link.at(-1, 0))
        edge_copy(marks.at[:HALF_ROWS, :EDGE], r.marks_corner, link.at(-1, -1))
    fill_table(upper, lower)

    def flip(source):
        for col in range(width // LANES):
            part = source[:total, col * LANES : (col + 1) * LANES]
            flipped[col * LANES : (col + 1) * LANES, :] = part.astype(BF16).T

    def weight_grad(name, right):
        def tile(place):
            put(name, cols_at(place), dot_nn(flipped[...], right[:, cols_at(place)].astype(BF16)))

        loop(right.shape[1] // TILE, tile)

    device_row = lax.axis_index("lat") * row_count + HALF_ROWS

    def units(place):
        return [(place * group + part, pair) for part in range(group) for pair in range(pairs)]

    def attend(place):
        place_q = lax.broadcasted_iota(jnp.int32, (TOKENS, TOKENS), 0)
        place_k = lax.broadcasted_iota(jnp.int32, (TOKENS, TOKENS), 1)
        bias = {}
        for part in range(group):
            window = place * group + part
            limit = (row_total - device_row - (window // across) * WIN_LAT) * WIN_LON
            alike = jnp.where((place_q >= limit) == (place_k >= limit), 0.0, masked)
            bias[part] = jnp.concatenate([alike, alike], 0)
        scores = []
        for index, (window, pair) in enumerate(units(place)):
            rows, start = rows_at(window, TOKENS), pair * LANES
            query = pair_stack(qkv[rows, start : start + LANES])
            key = qkv[rows, width + start : width + start + LANES].astype(BF16)
            scores.append(dot_nt(query, key) + bias[index // pairs])
        for score, (window, pair) in zip(scores, units(place)):
            exponent = jnp.exp2((score - jnp.max(score, -1, keepdims=True)) * SOFTMAX_SCALE)
            probs[window * pairs + pair] = exponent * (1.0 / jnp.sum(exponent, -1, keepdims=True))
        for window, pair in units(place):
            rows, start = rows_at(window, TOKENS), pair * LANES
            value = qkv[rows, 2 * width + start : 2 * width + start + LANES].astype(BF16)
            chance = probs[window * pairs + pair].astype(BF16)
            context[rows, start : start + LANES] = pair_merge(dot_nn(chance, value))

    half = across * TOKENS
    half_block = row_block(half, 288)

    def first_norm(place):
        rows = rows_at(place, half_block)
        normed1[rows] = normalize(latent[rows])[0].astype(BF16)

    def project(part, place):
        rows = slice(part * half, (part + 1) * half)
        qkv[rows, cols_at(place)] = dot_nn(normed1[rows], w_qkv[:, cols_at(place)])

    parts = row_count // WIN_LAT
    for part in range(parts):
        if part == 0:
            arrived(0)
        if part == parts - 1:
            arrived(1, 2)
        cut_windows(part, main, r.east, r.south, r.corner, strip_in, latent)
        steps = half // half_block
        loop(steps, lambda place: first_norm(part * steps + place))
        if part == 0:
            arrivals[0].wait()
        loop(3 * width // TILE, lambda place: project(part, place))
        groups = across // group
        loop(groups, lambda place: attend(part * groups + place))

    def after_attention(place):
        rows = rows_at(place, block)
        attended = dot_nn(context[rows].astype(BF16), w_proj[...]).astype(BF16)
        summed = latent[rows] + attended.astype(F32)
        residual[rows] = summed
        normed2[rows] = normalize(summed)[0].astype(BF16)

    arrivals[1].wait()
    loop(blocks, after_attention)

    def widen(place):
        cols = cols_at(place // wide_blocks)
        rows = rows_at(place % wide_blocks, wide)
        pre_act = dot_nn(normed2[rows], w_fc1[:, cols])
        cdf = 0.5 * (1.0 + lax.erf(pre_act * (1.0 / math.sqrt(2.0))))
        density = jnp.exp2(pre_act * pre_act * (-0.5 / math.log(2.0))) * (1.0 / math.sqrt(2.0 * math.pi))
        activated[rows, cols] = (pre_act * cdf).astype(BF16)
        slope[rows, cols] = cdf + pre_act * density

    arrivals[2].wait()
    loop(wide_blocks * (ff // TILE), widen)

    def narrow(place):
        rows = rows_at(place, block)
        out = residual[rows] + dot_nn(activated[rows], w_fc2[...])
        block_out[rows] = out
        normed3[rows] = normalize(out)[0].astype(BF16)

    arrivals[3].wait()
    loop(blocks, narrow)

    def head(place):
        rows = rows_at(place, block)
        mark = marks_win[rows]
        weight_tok = mark[:, VARS : VARS + 1] / VARS
        bins = lax.broadcasted_iota(jnp.int32, (block, BINS), 1).astype(F32)
        for var in range(VARS):
            logits = dot_nn(normed3[rows], w_head[:, var * BINS : (var + 1) * BINS])
            exponent = jnp.exp(logits - jnp.max(logits, -1, keepdims=True))
            chance = exponent * (1.0 / jnp.sum(exponent, -1, keepdims=True))
            picked = jnp.where(mark[:, var : var + 1] == bins, 1.0, 0.0).astype(BF16)
            target = dot_nn(picked, upper[...]) + dot_nn(picked, lower[...])
            d_logits[rows, var * BINS : (var + 1) * BINS] = (weight_tok * (chance - target)).astype(BF16)

    arrived(3, 4, 5)
    for part in range(parts):
        cut_windows(part, marks, r.marks_east, r.marks_south, r.marks_corner, r.marks_strip, marks_win)
    arrivals[4].wait()
    loop(blocks, head)

    flip(normed3)
    weight_grad("head", d_logits)
    advance("head", Summed.start)
    d_outb = normed3

    def head_back(place):
        rows = rows_at(place, block)
        scaled, inverse = normalize(block_out[rows])
        back = norm_back(scaled, inverse, dot_nt(d_logits[rows], w_head[...]))
        d_out[rows] = back
        d_outb[rows] = back.astype(BF16)

    loop(blocks, head_back)
    advance("head", Summed.spread)

    fc2_rows = 4 * ff // (lats * lons) if linked else TILE

    def grad_narrow(place):
        grad = dot_nn(activated[:, cols_at(place, fc2_rows)].T, d_outb[...]).astype(BF16)
        if linked:
            whole = sums["fc2"].whole
            whole[place // 2, place % 2] = grad.reshape(*whole.shape[2:])
        else:
            r.g_fc2[rows_at(place, fc2_rows)] = grad

    loop(ff // fc2_rows, grad_narrow)
    advance("fc2", Summed.start)
    advance("head", Summed.cross)

    d_pre = slope

    def widen_back(place):
        cols = cols_at(place)
        back = dot_nt(d_outb[...], w_fc2[rows_at(place, TILE)])
        d_pre[:, cols] = back * slope[:, cols]

    loop(ff // TILE, widen_back)
    advance("fc2", Summed.spread)
    advance("head", Summed.deal)

    flip(normed2)
    weight_grad("fc1", d_pre)
    advance("fc1", Summed.start)

    d_attended = d_outb
    d_resid = d_out

    def residual_back(place):
        rows = rows_at(place, block)
        scaled, inverse = normalize(residual[rows])
        back = d_out[rows] + norm_back(scaled, inverse, dot_nt(d_pre[rows].astype(BF16), w_fc1[...]))
        d_resid[rows] = back
        d_attended[rows] = back.astype(BF16)

    loop(blocks, residual_back)
    advance("fc2", Summed.cross)
    advance("fc1", Summed.spread)

    flip(context)
    weight_grad("proj", d_attended)
    advance("proj", Summed.start)
    advance("head", Summed.finish)

    d_context = context

    def context_back(place):
        rows = rows_at(place, block)
        d_context[rows] = dot_nt(d_attended[rows], w_proj[...])

    loop(blocks, context_back)
    advance("proj", Summed.spread)

    def attend_back(place):
        d_probs = []
        for window, pair in units(place):
            rows, start = rows_at(window, TOKENS), pair * LANES
            upstream = pair_stack(d_context[rows, start : start + LANES])
            at_v = slice(2 * width + start, 2 * width + start + LANES)
            d_probs.append(dot_nt(upstream, qkv[rows, at_v].astype(BF16)))
            chance_t = probs[window * pairs + pair].T.astype(BF16)
            qkv[rows, at_v] = dot_nn(chance_t, upstream)
        for d_prob, (window, pair) in zip(d_probs, units(place)):
            rows, start = rows_at(window, TOKENS), pair * LANES
            at_q, at_k = slice(start, start + LANES), slice(width + start, width + start + LANES)
            query = pair_stack(qkv[rows, at_q])
            key = qkv[rows, at_k].astype(BF16)
            chance = probs[window * pairs + pair]
            inner = jnp.sum(d_prob * chance, -1, keepdims=True)
            d_scores = chance * (d_prob - inner) * HEAD_DIM ** (-0.5)
            qkv[rows, at_q] = pair_merge(dot_nn(d_scores.astype(BF16), key))
            qkv[rows, at_k] = dot_nn(d_scores.T.astype(BF16), query)

    def some_windows(first, last):
        loop(last - first, lambda window: attend_back(first + window))

    groups = windows // group
    some_windows(0, groups // 3)
    advance("fc2", Summed.deal)
    some_windows(groups // 3, groups)
    advance("fc1", Summed.cross)

    flip(normed1)
    weight_grad("qkv", qkv)
    advance("qkv", Summed.start)
    advance("proj", Summed.cross)
    advance("fc2", Summed.finish)

    def latent_back(place):
        rows = rows_at(place, block)
        d_shifted = dot_nt(qkv[rows].astype(BF16), w_qkv[...]).astype(BF16)
        scaled, inverse = normalize(latent[rows])
        block_out[rows] = d_resid[rows] + norm_back(scaled, inverse, d_shifted.astype(F32))

    loop(blocks, latent_back)
    advance("qkv", Summed.spread)
    advance("fc1", Summed.deal)
    join_windows(block_out, strip, row_count, col_count)
    if not linked:
        for row in range(row_count):
            r.g_main[row] = strip[row * pitch : row * pitch + col_count].astype(BF16)
            r.g_edge[row] = strip[row * pitch + col_count : (row + 1) * pitch].astype(BF16)
        return

    own_rows = row_count - HALF_ROWS
    pad = jnp.zeros((EDGE, width), F32)
    for row in range(row_count):
        edge = jnp.concatenate([strip[row * pitch + col_count : (row + 1) * pitch], pad], 0)
        if row < own_rows:
            r.to_east[row] = edge.astype(BF16)
        else:
            r.to_corner[row - own_rows] = edge.astype(BF16)
            r.to_south[row - own_rows] = strip[row * pitch : row * pitch + col_count].astype(BF16)
    first_back = len(edge_copies)
    edge_copy(r.to_east, r.from_west, link.at(0, 1))
    edge_copy(r.to_south, r.from_north, link.at(1, 0))
    edge_copy(r.to_corner, r.from_corner, link.at(1, 1))

    advance("proj", Summed.deal)
    advance("qkv", Summed.cross)
    advance("fc1", Summed.finish)
    ours = lax.broadcasted_iota(jnp.int32, (EDGE, width), 0) >= HALF_COLS

    def put_row(row, body, edge):
        head = jnp.where(ours, body[:EDGE], edge[:EDGE])
        r.g_main[row] = jnp.concatenate([head, body[EDGE:]], 0).astype(BF16)

    advance("qkv", Summed.deal)
    for made in edge_copies[first_back:]:
        made.wait_recv()
    for row in range(own_rows):
        body = strip[row * pitch : row * pitch + col_count]
        put_row(row + HALF_ROWS, body, r.from_west[row].astype(F32))
    for row in range(HALF_ROWS):
        put_row(row, r.from_north[row].astype(F32), r.from_corner[row].astype(F32))
    advance("proj", Summed.finish)
    advance("qkv", Summed.finish)
    for made in edge_copies:
        made.wait_send()
    for name in GRADS:
        sums[name].drain()


GRADS = ("qkv", "proj", "fc1", "fc2", "head")


def device_step(latent, edges, target, land, marks_edges, weights, lats, lons, linked):
    row_count, col_count, width = latent.shape
    total = row_count * col_count
    windows = total // TOKENS
    ff = weights[2].shape[1]
    padded = row_count * (col_count + EDGE)
    ins = dict(main=latent, target=target.transpose(0, 2, 1), land=land)
    if not linked:
        ins |= dict(zip(("east", "south", "corner"), edges))
        ins |= dict(zip(("marks_east", "marks_south", "marks_corner"), marks_edges))
    near = len(ins)
    ins |= {f"weight{place}": weight for place, weight in enumerate(weights)}
    outs = dict(g_main=jax.ShapeDtypeStruct((row_count, col_count, width), BF16))
    if not linked:
        outs |= dict(g_edge=jax.ShapeDtypeStruct((row_count, EDGE, width), BF16))
    for name, weight in zip(GRADS, weights):
        rows = weight.shape[0] // (lats * lons if linked else 1)
        outs["g_" + name] = jax.ShapeDtypeStruct((rows, weight.shape[1]), F32 if linked else BF16)
    scratch = {f"held{place}": pltpu.VMEM(weight.shape, BF16) for place, weight in enumerate(weights)}
    scratch |= dict(
        weight_sem=pltpu.SemaphoreType.DMA((len(weights),)),
        marks=pltpu.VMEM((row_count, col_count, LANES), F32),
        marks_strip=pltpu.VMEM((padded, LANES), F32),
        latent=pltpu.VMEM((total, width), F32),
        marks_win=pltpu.VMEM((total, LANES), F32),
        normed1=pltpu.VMEM((total, width), BF16),
        qkv=pltpu.VMEM((total, 3 * width), F32),
        probs=pltpu.VMEM((windows * (width // LANES), 2 * TOKENS, TOKENS), F32),
        context=pltpu.VMEM((padded, width), F32),
        residual=pltpu.VMEM((padded, width), F32),
        normed2=pltpu.VMEM((total, width), BF16),
        activated=pltpu.VMEM((total, ff), BF16),
        slope=pltpu.VMEM((total, ff), F32),
        block_out=pltpu.VMEM((total, width), F32),
        normed3=pltpu.VMEM((total, width), BF16),
        d_logits=pltpu.VMEM((total, VARS * BINS), BF16),
        d_out=pltpu.VMEM((total, width), F32),
        flipped=pltpu.VMEM((width, total), BF16),
        upper=pltpu.VMEM((BINS, BINS), BF16),
        lower=pltpu.VMEM((BINS, BINS), BF16),
    )
    if linked:
        own_rows = row_count - HALF_ROWS
        wide, high, both = (row_count, 2 * EDGE), (HALF_ROWS, col_count), (HALF_ROWS, 2 * EDGE)
        own = (own_rows, 2 * EDGE)
        scratch |= dict(
            east=pltpu.VMEM((*wide, width), BF16),
            south=pltpu.VMEM((*high, width), BF16),
            corner=pltpu.VMEM((*both, width), BF16),
            marks_east=pltpu.VMEM((row_count, EDGE, LANES), F32),
            marks_south=pltpu.VMEM((*high, LANES), F32),
            marks_corner=pltpu.VMEM((HALF_ROWS, EDGE, LANES), F32),
            to_east=pltpu.VMEM((*own, width), BF16),
            to_south=pltpu.VMEM((*high, width), BF16),
            to_corner=pltpu.VMEM((*both, width), BF16),
            from_west=pltpu.VMEM((*own, width), BF16),
            from_north=pltpu.VMEM((*high, width), BF16),
            from_corner=pltpu.VMEM((*both, width), BF16),
            edge_send=pltpu.SemaphoreType.DMA((9,)),
            edge_recv=pltpu.SemaphoreType.DMA((9,)),
        )
        for name, weight in zip(GRADS, weights):
            rows, cols = weight.shape[0] // (lats * lons), weight.shape[1]
            stages = [
                pltpu.VMEM((lats, 2, 2, 2, rows, cols), BF16),
                pltpu.VMEM((lats, 2, 2, rows, cols), BF16),
                pltpu.VMEM((lats, 2, rows, cols // 2), BF16),
                pltpu.VMEM((lats, 2, rows, cols // 2), BF16),
                pltpu.VMEM((lats, rows, cols), BF16),
                pltpu.VMEM((lats - 1, rows, cols), BF16),
                pltpu.SemaphoreType.DMA((4 + lats,)),
                pltpu.SemaphoreType.DMA((4 + lats,)),
            ]
            scratch |= {f"{name}{place}": stage for place, stage in enumerate(stages)}
    vmem = pl.BlockSpec(memory_space=pltpu.VMEM)
    names = [*ins, *outs, *scratch]
    done = pl.pallas_call(
        functools.partial(step_kernel, row_count * lats, lats, lons, linked, names),
        in_specs=[vmem] * near + [pl.BlockSpec(memory_space=pl.ANY)] * len(weights),
        out_specs=[vmem] * len(outs),
        out_shape=list(outs.values()),
        scratch_shapes=list(scratch.values()),
        compiler_params=pltpu.CompilerParams(
            vmem_limit_bytes=67043328,
            **(dict(collective_id=0, has_side_effects=True) if linked else {}),
        ),
        cost_estimate=pl.CostEstimate(flops=20_000_000_000, bytes_accessed=20_000_000, transcendentals=0),
        name="device_step",
    )(*ins.values())
    return settled(done) if linked else done


def settle_kernel(count, *refs):
    for source, target in zip(refs[:count], refs[count:]):
        target[...] = source[...]


def settled(arrays):
    vmem = pl.BlockSpec(memory_space=pltpu.VMEM)
    return pl.pallas_call(
        functools.partial(settle_kernel, len(arrays)),
        in_specs=[vmem] * len(arrays),
        out_specs=[vmem] * len(arrays),
        out_shape=[jax.ShapeDtypeStruct(array.shape, array.dtype) for array in arrays],
        name="settle",
    )(*arrays)


def moved(value, axis, steps):
    count = lax.axis_size(axis)
    pairs = [(source, (source + steps) % count) for source in range(count)]
    return lax.ppermute(value, axis, pairs)


def edges_ahead(block):
    east = moved(block[:, :EDGE], "lon", -1)
    south = moved(block[:HALF_ROWS], "lat", -1)
    return east, south, moved(east[:HALF_ROWS], "lat", -1)


def roll_behind(body, edge):
    own_rows = body.shape[0] - HALF_ROWS
    west = moved(edge, "lon", 1)[:, :HALF_COLS]
    whole = jnp.concatenate([west, body[:, HALF_COLS:]], 1)
    north = moved(whole[own_rows:], "lat", 1)
    return jnp.concatenate([north, whole[:own_rows]], 0)


def scatter_over(value, axis):
    return lax.psum_scatter(value, axis, scatter_dimension=0, tiled=True)


def local(latent, w_qkv, w_proj, w_fc1, w_fc2, w_head, target_bins, land_mask):
    width = latent.shape[2]
    lats, lons = lax.axis_size("lat"), lax.axis_size("lon")
    devices = lats * lons
    linked = lons == 8 and lats > 2 and width % (16 * devices) == 0
    weights = (w_qkv, w_proj, w_fc1, w_fc2, w_head)
    if linked:
        return tuple(device_step(latent, (), target_bins, land_mask, (), weights, lats, lons, True))
    marks = jnp.concatenate([target_bins, land_mask[:, :, None]], 2).astype(F32)
    marks = jnp.pad(marks, ((0, 0), (0, 0), (0, LANES - marks.shape[2])))
    body, edge, *grads = device_step(
        latent, edges_ahead(latent), target_bins, land_mask, edges_ahead(marks), weights, lats, lons, False
    )
    grad_latent = roll_behind(body, edge)

    def to_columns(grad):
        deep = grad.shape[0] // width
        parts = grad.reshape(devices, deep, width // devices, -1)
        return [parts[:, part].reshape(width, -1) for part in range(deep)]

    columns = [to_columns(grad) for grad in grads]
    joined = jnp.concatenate([part for group in columns for part in group], 1)
    summed = scatter_over(scatter_over(joined, "lat"), "lon").astype(F32)
    outs, start = [], 0
    for grad, group in zip(grads, columns):
        size = grad.shape[1]
        pieces = [summed[:, start + part * size : start + (part + 1) * size] for part in range(len(group))]
        outs.append(jnp.concatenate(pieces, 0))
        start += size * len(group)
    return (grad_latent, *outs)


def solution(mesh):
    grid = P("lat", "lon", None)
    spread = P(("lat", "lon"), None)
    return jax.shard_map(
        local,
        mesh=mesh,
        in_specs=(grid, P(), P(), P(), P(), P(), grid, P("lat", "lon")),
        out_specs=(grid, spread, spread, spread, spread, spread),
        check_vma=False,
    )
```

```python
import functools
import math
import types

import jax
import jax.numpy as jnp
from jax import lax
from jax.experimental import pallas as pl
from jax.experimental.pallas import tpu as pltpu
from jax.sharding import PartitionSpec as P

HEADS = 8
BINS = 256
VARS = 4
WIN_LAT = 6
WIN_LON = 12
HEAD_DIM = 64
TOKENS = WIN_LAT * WIN_LON
HALF_ROWS = WIN_LAT // 2
HALF_COLS = WIN_LON // 2
EDGE = 8
LANES = 128
TILE = 256

eps = 1e-05
smear = 0.75
masked = -1e30
SOFTMAX_SCALE = HEAD_DIM ** (-0.5) / math.log(2.0)

F32 = jnp.float32
BF16 = jnp.bfloat16


def dot_nn(left, right):
    return lax.dot_general(left, right, (((1,), (0,)), ((), ())), preferred_element_type=F32)


def dot_nt(left, right):
    return lax.dot_general(left, right, (((1,), (1,)), ((), ())), preferred_element_type=F32)


def normalize(values_in):
    centre = jnp.mean(values_in, -1, keepdims=True)
    offset = values_in - centre
    inverse = lax.rsqrt(jnp.mean(offset * offset, -1, keepdims=True) + eps)
    return (offset * inverse, inverse)


def norm_back(scaled, inverse, upstream):
    return inverse * (
        upstream
        - jnp.mean(upstream, -1, keepdims=True)
        - scaled * jnp.mean(upstream * scaled, -1, keepdims=True)
    )


def loop(count, body):
    def step(place, carry):
        body(place)
        return carry

    lax.fori_loop(0, count, step, 0)


def loop_from(first, last, body):
    loop(last - first, lambda place: body(first + place))


def rows_at(place, size):
    return pl.ds(pl.multiple_of(place * size, math.gcd(size, 16)), size)


def cols_at(place, size=TILE):
    return pl.ds(pl.multiple_of(place * size, size), size)


def row_block(count, most):
    best = 16
    for size in range(16, most + 1, 16):
        if count % size == 0:
            best = size
    return best


def pair_stack(block):
    lane = lax.broadcasted_iota(jnp.int32, block.shape, 1)
    low = lane < HEAD_DIM
    return jnp.concatenate([jnp.where(low, block, 0.0), jnp.where(low, 0.0, block)], 0).astype(BF16)


def pair_merge(stacked):
    top, bottom = stacked[:TOKENS], stacked[TOKENS:]
    lane = lax.broadcasted_iota(jnp.int32, top.shape, 1)
    return jnp.where(lane < HEAD_DIM, top, bottom)


def lay_rows(rows, main, east, south, corner, strip, bodies, edges):
    row_count, col_count = main.shape[0], main.shape[1]
    own_rows, pitch = row_count - HALF_ROWS, col_count + EDGE
    for row in rows:
        if row < own_rows:
            body, edge = main.at[row + HALF_ROWS], east.at[row]
        else:
            body, edge = south.at[row - own_rows], corner.at[row - own_rows]
        if bodies:
            strip[row * pitch : row * pitch + col_count] = body[...].astype(F32)
        if edges:
            strip[row * pitch + col_count : (row + 1) * pitch] = edge[...].astype(F32)[:EDGE]


def cut_windows(first, last, col_count, strip, wins):
    across, pitch = col_count // WIN_LON, col_count + EDGE
    for window in range(first, last):
        for row in range(WIN_LAT):
            start = window * TOKENS + row * WIN_LON
            source = (window // across * WIN_LAT + row) * pitch + HALF_COLS + window % across * WIN_LON
            wins[start : start + WIN_LON] = strip[source : source + WIN_LON]


def join_windows(part, wins, strip, col_count):
    across, pitch = col_count // WIN_LON, col_count + EDGE
    for row in range(part * WIN_LAT, (part + 1) * WIN_LAT):
        for col in range(across):
            start = (part * across + col) * TOKENS + row % WIN_LAT * WIN_LON
            target = row * pitch + HALF_COLS + col * WIN_LON
            strip[target : target + WIN_LON] = wins[start : start + WIN_LON]


def fill_table(upper, lower):
    scale = smear * math.sqrt(2.0)

    def mass_below(edge, centre):
        return 0.5 * lax.erf((edge - centre) / scale)

    def part(place):
        base = place * 64
        centre = (base + lax.broadcasted_iota(jnp.int32, (64, BINS), 0)).astype(F32) + 0.5
        edge = lax.broadcasted_iota(jnp.int32, (64, BINS), 1).astype(F32)
        whole = mass_below(float(BINS), centre) - mass_below(0.0, centre)
        table = (mass_below(edge + 1.0, centre) - mass_below(edge, centre)) / whole
        high = table.astype(BF16)
        upper[pl.ds(pl.multiple_of(base, 64), 64)] = high
        lower[pl.ds(pl.multiple_of(base, 64), 64)] = (table - high.astype(F32)).astype(BF16)

    loop(BINS // 64, part)


class Summed:
    def __init__(self, link, refs, out, cols):
        self.link, self.out, self.cols = link, out, cols
        self.whole, self.pair, self.first, self.second, self.plane, self.slots = refs[:6]
        self.semaphores = refs[6:]
        self.half = self.plane.shape[-1] // 2
        self.copies = []

    def copy(self, place, source, target, where):
        send, recv = self.semaphores
        made = pltpu.make_async_remote_copy(
            src_ref=source, dst_ref=target, send_sem=send.at[place], recv_sem=recv.at[place],
            device_id=where, device_id_type=pl.DeviceIdType.MESH,
        )
        made.start()
        self.copies.append(made)

    def start(self):
        link = self.link
        self.copy(0, self.whole.at[:, :, :, 1 - link.core], self.pair, link.over(1))

    def spread(self):
        link, half = self.link, self.half
        self.copies[0].wait_recv()

        def add(row):
            self.pair[row] = self.pair[row] + self.whole[row, :, :, link.core]

        loop(self.pair.shape[0], add)
        self.copy(1, self.pair.at[:, :, 1 - link.x, :, :half], self.first, link.over(2))
        self.copy(2, self.pair.at[:, 1 - link.y, :, :, half:], self.second, link.over(4))

    def cross(self):
        link, half = self.link, self.half
        self.copies[1].wait_recv()

        def add_first(row):
            self.first[row] = self.first[row] + self.pair[row, :, link.x, :, :half]

        loop(self.pair.shape[0], add_first)
        self.copy(3, self.first.at[:, 1 - link.y], self.plane.at[:, :, :half], link.over(4))
        self.copies[2].wait_recv()

        def add_second(row):
            self.second[row] = self.second[row] + self.pair[row, link.y, :, :, half:]

        loop(self.pair.shape[0], add_second)
        self.copy(4, self.second.at[:, 1 - link.x], self.plane.at[:, :, half:], link.over(2))

    def deal(self):
        link, half = self.link, self.half
        self.copies[3].wait_recv()
        self.copies[4].wait_recv()

        def add(row):
            self.plane[row, :, :half] = self.plane[row, :, :half] + self.first[row, link.y]
            self.plane[row, :, half:] = self.plane[row, :, half:] + self.second[row, link.x]

        loop(self.plane.shape[0], add)
        for step in range(1, link.lats):
            there = lax.rem(link.lat + step, link.lats)
            self.copy(4 + step, self.plane.at[there], self.slots.at[step - 1], (there, link.lon))

    def finish(self):
        link = self.link
        total = self.plane[link.lat].astype(F32)
        for step in range(1, link.lats):
            self.copies[4 + step].wait_recv()
            total = total + self.slots[step - 1].astype(F32)
        self.out[:, self.cols] = total

    def drain(self):
        for made in self.copies:
            made.wait_send()


class Link:
    def __init__(self, lats, lons):
        self.lats, self.lons = lats, lons
        self.lat, self.lon = lax.axis_index("lat"), lax.axis_index("lon")
        self.core = lax.rem(self.lon, 2)
        self.x = lax.rem(self.lon // 2, 2)
        self.y = lax.rem(self.lon // 4, 2)

    def over(self, step):
        bit = lax.rem(self.lon // step, 2)
        return (self.lat, self.lon + step - 2 * step * bit)

    def at(self, north, west):
        return (
            lax.rem(self.lat + self.lats + north, self.lats),
            lax.rem(self.lon + self.lons + west, self.lons),
        )

    def greet(self):
        barrier = pltpu.get_barrier_semaphore()
        peers = [self.over(1), self.over(2), self.over(4)]
        peers += [self.at(step, 0) for step in range(1, self.lats)]
        peers += [self.at(0, 1), self.at(0, -1), self.at(1, 1), self.at(-1, -1)]
        for peer in peers:
            pl.semaphore_signal(barrier, inc=1, device_id=peer, device_id_type=pl.DeviceIdType.MESH)
        pl.semaphore_wait(barrier, len(peers))


def step_kernel(row_total, lats, lons, linked, names, *refs):
    r = types.SimpleNamespace(**dict(zip(names, refs)))
    main, marks = r.main, r.marks
    w_qkv, w_proj, w_fc1, w_fc2, w_head = (getattr(r, f"held{place}") for place in range(5))
    arrivals = [
        pltpu.make_async_copy(getattr(r, f"weight{place}"), getattr(r, f"held{place}"), r.weight_sem.at[place])
        for place in range(5)
    ]
    for place in (0, 1, 2, 3, 4):
        arrivals[place].start()
    latent, marks_win, normed1, qkv, probs = r.latent, r.marks_win, r.normed1, r.qkv, r.probs
    context, residual, normed2, activated = r.context, r.residual, r.normed2, r.activated
    slope, block_out, normed3, d_logits = r.slope, r.block_out, r.normed3, r.d_logits
    d_out, flipped, upper, lower = r.d_out, r.flipped, r.upper, r.lower
    strip_in = r.residual
    strip_out = r.strip_out
    row_count, col_count, width = main.shape
    total = row_count * col_count
    windows = total // TOKENS
    across = col_count // WIN_LON
    pairs = width // LANES
    group = 2 - across % 2
    block = row_block(total, 288)
    blocks = total // block
    wide = row_block(total, 448)
    wide_blocks = total // wide
    ff = w_fc1.shape[1]
    pitch = col_count + EDGE

    edge_copies, sums = [], {}
    if linked:
        link = Link(lats, lons)
        link.greet()

        def edge_copy(source, target, where):
            place = len(edge_copies)
            made = pltpu.make_async_remote_copy(
                src_ref=source, dst_ref=target, send_sem=r.edge_send.at[place],
                recv_sem=r.edge_recv.at[place], device_id=where,
                device_id_type=pl.DeviceIdType.MESH,
            )
            made.start()
            edge_copies.append(made)

        edge_copy(main.at[:HALF_ROWS, : 2 * EDGE], r.corner, link.at(-1, -1))
        edge_copy(main.at[:HALF_ROWS], r.south, link.at(-1, 0))
        edge_copy(main.at[HALF_ROWS:, : 2 * EDGE], r.east, link.at(0, -1))
        for name, parts in GRADS:
            out = getattr(r, "g_" + name)
            for part in range(parts):
                size = out.shape[1] // parts
                refs = [getattr(r, f"{name}{part}_{place}") for place in range(8)]
                sums[name, part] = Summed(link, refs, out, slice(part * size, (part + 1) * size))

    def advance(name, part, stage):
        if linked:
            stage(sums[name, part])

    def arrived(*places):
        for place in places:
            if linked:
                edge_copies[place].wait_recv()

    def fill_marks(row):
        pad = jnp.zeros((8 - VARS - 1, col_count), F32)
        bins, land = r.target[row].astype(F32), r.land[row : row + 1].astype(F32)
        marks[row, :, :8] = jnp.concatenate([bins, land, pad], 0).T

    for row in range(row_count):
        fill_marks(row)
    fill_table(upper, lower)

    def flip(source):
        for col in range(width // LANES):
            part = source[:total, col * LANES : (col + 1) * LANES]
            flipped[col * LANES : (col + 1) * LANES, :] = part.astype(BF16).T

    def weight_grad(name, part, right):
        tiles = right.shape[1] // TILE // dict(GRADS)[name]

        def tile(place):
            cols = cols_at(part * tiles + place)
            grad = dot_nn(flipped[...], right[:, cols].astype(BF16)).astype(BF16)
            if linked:
                whole = sums[name, part].whole
                whole[:, :, :, :, :, cols_at(place)] = grad.reshape(*whole.shape[:5], TILE)
            else:
                getattr(r, "g_" + name)[:, cols] = grad

        loop(tiles, tile)
        advance(name, part, Summed.start)

    device_row = lax.axis_index("lat") * row_count + HALF_ROWS

    def units(place):
        return [(place * group + part, pair) for part in range(group) for pair in range(pairs)]

    def attend(place):
        place_q = lax.broadcasted_iota(jnp.int32, (TOKENS, TOKENS), 0)
        place_k = lax.broadcasted_iota(jnp.int32, (TOKENS, TOKENS), 1)
        bias = {}
        for part in range(group):
            window = place * group + part
            limit = (row_total - device_row - (window // across) * WIN_LAT) * WIN_LON
            alike = jnp.where((place_q >= limit) == (place_k >= limit), 0.0, masked)
            bias[part] = jnp.concatenate([alike, alike], 0)
        scores = []
        for index, (window, pair) in enumerate(units(place)):
            rows, start = rows_at(window, TOKENS), pair * LANES
            query = pair_stack(qkv[rows, start : start + LANES])
            key = qkv[rows, width + start : width + start + LANES].astype(BF16)
            scores.append(dot_nt(query, key) + bias[index // pairs])
        for score, (window, pair) in zip(scores, units(place)):
            exponent = jnp.exp2((score - jnp.max(score, -1, keepdims=True)) * SOFTMAX_SCALE)
            probs[window * pairs + pair] = exponent * (1.0 / jnp.sum(exponent, -1, keepdims=True))
        for window, pair in units(place):
            rows, start = rows_at(window, TOKENS), pair * LANES
            value = qkv[rows, 2 * width + start : 2 * width + start + LANES].astype(BF16)
            chance = probs[window * pairs + pair].astype(BF16)
            context[rows, start : start + LANES] = pair_merge(dot_nn(chance, value))

    def first_norm(place):
        rows = rows_at(place, TOKENS * group)
        normed1[rows] = normalize(latent[rows])[0].astype(BF16)

    def project(rows, place):
        qkv[rows, cols_at(place)] = dot_nn(normed1[rows], w_qkv[:, cols_at(place)])

    def forward_windows(first, last):
        loop_from(first // group, last // group, first_norm)
        rows = slice(first * TOKENS, last * TOKENS)
        loop(3 * width // TILE, lambda place: project(rows, place))
        loop_from(first // group, last // group, attend)

    grid_refs = (main, r.east, r.south, r.corner, strip_in)
    own_rows = row_count - HALF_ROWS
    lay_rows(range(own_rows), *grid_refs, True, False)
    early = (across - 1) // group * group
    cut_windows(0, early, col_count, strip_in, latent)
    arrivals[0].wait()
    if early:
        forward_windows(0, early)
    arrived(0, 1, 2)
    if linked:
        edge_copy(marks.at[HALF_ROWS:, :EDGE], r.marks_east, link.at(0, -1))
        edge_copy(marks.at[:HALF_ROWS], r.marks_south, link.at(-1, 0))
        edge_copy(marks.at[:HALF_ROWS, :EDGE], r.marks_corner, link.at(-1, -1))
    lay_rows(range(own_rows), *grid_refs, False, True)
    lay_rows(range(own_rows, row_count), *grid_refs, True, True)
    cut_windows(early, windows, col_count, strip_in, latent)
    forward_windows(early, windows)

    def after_attention(place):
        rows = rows_at(place, block)
        attended = dot_nn(context[rows].astype(BF16), w_proj[...]).astype(BF16)
        summed = latent[rows] + attended.astype(F32)
        residual[rows] = summed
        normed2[rows] = normalize(summed)[0].astype(BF16)

    arrivals[1].wait()
    loop(blocks, after_attention)

    def widen(place):
        cols = cols_at(place // wide_blocks)
        rows = rows_at(place % wide_blocks, wide)
        pre_act = dot_nn(normed2[rows], w_fc1[:, cols])
        cdf = 0.5 * (1.0 + lax.erf(pre_act * (1.0 / math.sqrt(2.0))))
        density = jnp.exp2(pre_act * pre_act * (-0.5 / math.log(2.0))) * (1.0 / math.sqrt(2.0 * math.pi))
        activated[rows, cols] = (pre_act * cdf).astype(BF16)
        slope[rows, cols] = cdf + pre_act * density

    arrivals[2].wait()
    loop(wide_blocks * (ff // TILE), widen)

    def narrow(place):
        rows = rows_at(place, block)
        out = residual[rows] + dot_nn(activated[rows], w_fc2[...])
        block_out[rows] = out
        normed3[rows] = normalize(out)[0].astype(BF16)

    arrivals[3].wait()
    loop(blocks, narrow)

    def head(place):
        rows = rows_at(place, block)
        mark = marks_win[rows]
        weight_tok = mark[:, VARS : VARS + 1] / VARS
        bins = lax.broadcasted_iota(jnp.int32, (block, BINS), 1).astype(F32)
        for var in range(VARS):
            logits = dot_nn(normed3[rows], w_head[:, var * BINS : (var + 1) * BINS])
            exponent = jnp.exp(logits - jnp.max(logits, -1, keepdims=True))
            chance = exponent * (1.0 / jnp.sum(exponent, -1, keepdims=True))
            picked = jnp.where(mark[:, var : var + 1] == bins, 1.0, 0.0).astype(BF16)
            target = dot_nn(picked, upper[...]) + dot_nn(picked, lower[...])
            d_logits[rows, var * BINS : (var + 1) * BINS] = (weight_tok * (chance - target)).astype(BF16)

    arrived(3, 4, 5)
    lay_rows(range(row_count), marks, r.marks_east, r.marks_south, r.marks_corner, r.marks_strip, True, True)
    cut_windows(0, windows, col_count, r.marks_strip, marks_win)
    arrivals[4].wait()
    loop(blocks, head)

    flip(normed3)
    weight_grad("head", 0, d_logits)
    d_outb = normed3

    def head_back(place):
        rows = rows_at(place, block)
        scaled, inverse = normalize(block_out[rows])
        back = norm_back(scaled, inverse, dot_nt(d_logits[rows], w_head[...]))
        d_out[rows] = back
        d_outb[rows] = back.astype(BF16)

    loop(blocks, head_back)
    advance("head", 0, Summed.spread)

    fc2_parts = dict(GRADS)["fc2"]
    fc2_rows = 4 * ff // (lats * lons) if linked else TILE

    def grad_narrow(place):
        grad = dot_nn(activated[:, cols_at(place, fc2_rows)].T, d_outb[...]).astype(BF16)
        if not linked:
            r.g_fc2[rows_at(place, fc2_rows)] = grad
            return
        for part in range(fc2_parts):
            whole = sums["fc2", part].whole
            size = whole.shape[-1]
            whole[place // 2, place % 2] = grad[:, part * size : (part + 1) * size].reshape(*whole.shape[2:])

    loop(ff // fc2_rows, grad_narrow)
    for part in range(fc2_parts):
        advance("fc2", part, Summed.start)

    d_pre = slope

    def widen_back(place):
        cols = cols_at(place)
        back = dot_nt(d_outb[...], w_fc2[rows_at(place, TILE)])
        d_pre[:, cols] = back * slope[:, cols]

    tiles = ff // TILE
    loop_from(0, tiles // 4, widen_back)
    advance("head", 0, Summed.cross)
    loop_from(tiles // 4, tiles * 5 // 8, widen_back)
    advance("fc2", 0, Summed.spread)
    loop_from(tiles * 5 // 8, tiles, widen_back)
    advance("fc2", 1, Summed.spread)

    flip(normed2)
    weight_grad("fc1", 0, d_pre)
    advance("head", 0, Summed.deal)
    weight_grad("fc1", 1, d_pre)
    advance("fc2", 0, Summed.cross)
    advance("fc1", 0, Summed.spread)

    d_attended = d_outb
    d_resid = d_out

    def residual_back(place):
        rows = rows_at(place, block)
        scaled, inverse = normalize(residual[rows])
        back = d_out[rows] + norm_back(scaled, inverse, dot_nt(d_pre[rows].astype(BF16), w_fc1[...]))
        d_resid[rows] = back
        d_attended[rows] = back.astype(BF16)

    loop(blocks, residual_back)
    advance("fc2", 1, Summed.cross)
    advance("fc1", 1, Summed.spread)

    flip(context)
    weight_grad("proj", 0, d_attended)
    advance("fc2", 0, Summed.deal)
    advance("head", 0, Summed.finish)

    d_context = context

    def context_back(place):
        rows = rows_at(place, block)
        d_context[rows] = dot_nt(d_attended[rows], w_proj[...])

    loop(blocks, context_back)

    def attend_back(place):
        d_probs = []
        for window, pair in units(place):
            rows, start = rows_at(window, TOKENS), pair * LANES
            upstream = pair_stack(d_context[rows, start : start + LANES])
            at_v = slice(2 * width + start, 2 * width + start + LANES)
            d_probs.append(dot_nt(upstream, qkv[rows, at_v].astype(BF16)))
            chance_t = probs[window * pairs + pair].T.astype(BF16)
            qkv[rows, at_v] = dot_nn(chance_t, upstream)
        for d_prob, (window, pair) in zip(d_probs, units(place)):
            rows, start = rows_at(window, TOKENS), pair * LANES
            at_q, at_k = slice(start, start + LANES), slice(width + start, width + start + LANES)
            query = pair_stack(qkv[rows, at_q])
            key = qkv[rows, at_k].astype(BF16)
            chance = probs[window * pairs + pair]
            inner = jnp.sum(d_prob * chance, -1, keepdims=True)
            d_scores = chance * (d_prob - inner) * HEAD_DIM ** (-0.5)
            qkv[rows, at_q] = pair_merge(dot_nn(d_scores.astype(BF16), key))
            qkv[rows, at_k] = dot_nn(d_scores.T.astype(BF16), query)

    half = across * TOKENS
    parts = row_count // WIN_LAT
    pad = jnp.zeros((EDGE, width), F32)
    first_back = len(edge_copies)

    def latent_back(part):
        rows = slice(part * half, (part + 1) * half)
        d_shifted = dot_nt(qkv[rows].astype(BF16), w_qkv[...]).astype(BF16)
        scaled, inverse = normalize(latent[rows])
        block_out[rows] = d_resid[rows] + norm_back(scaled, inverse, d_shifted.astype(F32))
        join_windows(part, block_out, strip_out, col_count)
        for row in range(part * WIN_LAT, (part + 1) * WIN_LAT):
            body = strip_out[row * pitch : row * pitch + col_count]
            edge = strip_out[row * pitch + col_count : (row + 1) * pitch]
            if not linked:
                r.g_main[row] = body.astype(BF16)
                r.g_edge[row] = edge.astype(BF16)
                continue
            edge = jnp.concatenate([edge, pad], 0).astype(BF16)
            if row < own_rows:
                r.to_east[row] = edge
            else:
                r.to_corner[row - own_rows] = edge
                r.to_south[row - own_rows] = body.astype(BF16)

    last = (parts - 1) * across // group
    groups = windows // group
    third = (groups - last) // 3
    loop_from(last, last + third, attend_back)
    advance("fc1", 0, Summed.cross)
    loop_from(last + third, last + 2 * third, attend_back)
    advance("proj", 0, Summed.spread)
    advance("fc2", 1, Summed.deal)
    loop_from(last + 2 * third, groups, attend_back)
    latent_back(parts - 1)
    advance("fc1", 1, Summed.cross)
    if linked:
        edge_copy(r.to_south, r.from_north, link.at(1, 0))
        edge_copy(r.to_corner, r.from_corner, link.at(1, 1))
    loop_from(0, last * 2 // 3, attend_back)
    advance("fc1", 0, Summed.deal)
    loop_from(last * 2 // 3, last, attend_back)
    advance("proj", 0, Summed.cross)

    flip(normed1)
    weight_grad("qkv", 0, qkv)
    advance("fc1", 1, Summed.deal)
    weight_grad("qkv", 1, qkv)
    weight_grad("qkv", 2, qkv)
    advance("qkv", 0, Summed.spread)
    for part in range(parts - 1):
        latent_back(part)
    advance("qkv", 1, Summed.spread)
    advance("proj", 0, Summed.deal)
    advance("qkv", 2, Summed.spread)
    if not linked:
        return
    for part in range(2):
        advance("fc2", part, Summed.finish)
    advance("qkv", 0, Summed.cross)
    advance("qkv", 1, Summed.cross)
    advance("qkv", 2, Summed.cross)
    edge_copy(r.to_east, r.from_west, link.at(0, 1))
    advance("qkv", 0, Summed.deal)
    advance("qkv", 1, Summed.deal)
    advance("qkv", 2, Summed.deal)
    advance("fc1", 0, Summed.finish)
    ours = lax.broadcasted_iota(jnp.int32, (EDGE, width), 0) >= HALF_COLS

    def put_row(row, body, edge):
        head = jnp.where(ours, body[:EDGE], edge[:EDGE])
        r.g_main[row] = jnp.concatenate([head, body[EDGE:]], 0).astype(BF16)

    for made in edge_copies[first_back:]:
        made.wait_recv()
    for row in range(own_rows):
        body = strip_out[row * pitch : row * pitch + col_count]
        put_row(row + HALF_ROWS, body, r.from_west[row].astype(F32))
    for row in range(HALF_ROWS):
        put_row(row, r.from_north[row].astype(F32), r.from_corner[row].astype(F32))
    advance("fc1", 1, Summed.finish)
    advance("proj", 0, Summed.finish)
    for part in range(3):
        advance("qkv", part, Summed.finish)
    for made in edge_copies:
        made.wait_send()
    for one in sums.values():
        one.drain()


GRADS = (("qkv", 3), ("proj", 1), ("fc1", 2), ("fc2", 2), ("head", 1))


def device_step(latent, edges, target, land, marks_edges, weights, lats, lons, linked):
    row_count, col_count, width = latent.shape
    total = row_count * col_count
    windows = total // TOKENS
    ff = weights[2].shape[1]
    padded = row_count * (col_count + EDGE)
    ins = dict(main=latent, target=target.transpose(0, 2, 1), land=land)
    if not linked:
        ins |= dict(zip(("east", "south", "corner"), edges))
        ins |= dict(zip(("marks_east", "marks_south", "marks_corner"), marks_edges))
    near = len(ins)
    ins |= {f"weight{place}": weight for place, weight in enumerate(weights)}
    outs = dict(g_main=jax.ShapeDtypeStruct((row_count, col_count, width), BF16))
    if not linked:
        outs |= dict(g_edge=jax.ShapeDtypeStruct((row_count, EDGE, width), BF16))
    for (name, _), weight in zip(GRADS, weights):
        rows = weight.shape[0] // (lats * lons if linked else 1)
        outs["g_" + name] = jax.ShapeDtypeStruct((rows, weight.shape[1]), F32 if linked else BF16)
    scratch = {f"held{place}": pltpu.VMEM(weight.shape, BF16) for place, weight in enumerate(weights)}
    scratch |= dict(
        weight_sem=pltpu.SemaphoreType.DMA((len(weights),)),
        marks=pltpu.VMEM((row_count, col_count, LANES), F32),
        marks_strip=pltpu.VMEM((padded, LANES), F32),
        latent=pltpu.VMEM((total, width), F32),
        marks_win=pltpu.VMEM((total, LANES), F32),
        normed1=pltpu.VMEM((total, width), BF16),
        qkv=pltpu.VMEM((total, 3 * width), F32),
        probs=pltpu.VMEM((windows * (width // LANES), 2 * TOKENS, TOKENS), F32),
        context=pltpu.VMEM((total, width), F32),
        residual=pltpu.VMEM((padded, width), F32),
        normed2=pltpu.VMEM((total, width), BF16),
        activated=pltpu.VMEM((total, ff), BF16),
        slope=pltpu.VMEM((total, ff), F32),
        block_out=pltpu.VMEM((total, width), F32),
        strip_out=pltpu.VMEM((padded, width), F32),
        normed3=pltpu.VMEM((total, width), BF16),
        d_logits=pltpu.VMEM((total, VARS * BINS), BF16),
        d_out=pltpu.VMEM((total, width), F32),
        flipped=pltpu.VMEM((width, total), BF16),
        upper=pltpu.VMEM((BINS, BINS), BF16),
        lower=pltpu.VMEM((BINS, BINS), BF16),
    )
    if linked:
        own_rows = row_count - HALF_ROWS
        own, high, both = (own_rows, 2 * EDGE), (HALF_ROWS, col_count), (HALF_ROWS, 2 * EDGE)
        scratch |= dict(
            east=pltpu.VMEM((*own, width), BF16),
            south=pltpu.VMEM((*high, width), BF16),
            corner=pltpu.VMEM((*both, width), BF16),
            marks_east=pltpu.VMEM((own_rows, EDGE, LANES), F32),
            marks_south=pltpu.VMEM((*high, LANES), F32),
            marks_corner=pltpu.VMEM((HALF_ROWS, EDGE, LANES), F32),
            to_east=pltpu.VMEM((*own, width), BF16),
            to_south=pltpu.VMEM((*high, width), BF16),
            to_corner=pltpu.VMEM((*both, width), BF16),
            from_west=pltpu.VMEM((*own, width), BF16),
            from_north=pltpu.VMEM((*high, width), BF16),
            from_corner=pltpu.VMEM((*both, width), BF16),
            edge_send=pltpu.SemaphoreType.DMA((9,)),
            edge_recv=pltpu.SemaphoreType.DMA((9,)),
        )
        for (name, parts), weight in zip(GRADS, weights):
            rows, cols = weight.shape[0] // (lats * lons), weight.shape[1] // parts
            stages = [
                pltpu.VMEM((lats, 2, 2, 2, rows, cols), BF16),
                pltpu.VMEM((lats, 2, 2, rows, cols), BF16),
                pltpu.VMEM((lats, 2, rows, cols // 2), BF16),
                pltpu.VMEM((lats, 2, rows, cols // 2), BF16),
                pltpu.VMEM((lats, rows, cols), BF16),
                pltpu.VMEM((lats - 1, rows, cols), BF16),
                pltpu.SemaphoreType.DMA((4 + lats,)),
                pltpu.SemaphoreType.DMA((4 + lats,)),
            ]
            scratch |= {
                f"{name}{part}_{place}": stage for part in range(parts) for place, stage in enumerate(stages)
            }
    vmem = pl.BlockSpec(memory_space=pltpu.VMEM)
    names = [*ins, *outs, *scratch]
    done = pl.pallas_call(
        functools.partial(step_kernel, row_count * lats, lats, lons, linked, names),
        in_specs=[vmem] * near + [pl.BlockSpec(memory_space=pl.ANY)] * len(weights),
        out_specs=[vmem] * len(outs),
        out_shape=list(outs.values()),
        scratch_shapes=list(scratch.values()),
        compiler_params=pltpu.CompilerParams(
            vmem_limit_bytes=67043328,
            **(dict(collective_id=0, has_side_effects=True) if linked else {}),
        ),
        cost_estimate=pl.CostEstimate(flops=20_000_000_000, bytes_accessed=20_000_000, transcendentals=0),
        name="device_step",
    )(*ins.values())
    return settled(done) if linked else done


def settle_kernel(count, *refs):
    for source, target in zip(refs[:count], refs[count:]):
        target[...] = source[...]


def settled(arrays):
    vmem = pl.BlockSpec(memory_space=pltpu.VMEM)
    return pl.pallas_call(
        functools.partial(settle_kernel, len(arrays)),
        in_specs=[vmem] * len(arrays),
        out_specs=[vmem] * len(arrays),
        out_shape=[jax.ShapeDtypeStruct(array.shape, array.dtype) for array in arrays],
        name="settle",
    )(*arrays)


def moved(value, axis, steps):
    count = lax.axis_size(axis)
    pairs = [(source, (source + steps) % count) for source in range(count)]
    return lax.ppermute(value, axis, pairs)


def edges_ahead(block):
    east = moved(block[:, :EDGE], "lon", -1)
    south = moved(block[:HALF_ROWS], "lat", -1)
    return east[HALF_ROWS:], south, moved(east[:HALF_ROWS], "lat", -1)


def roll_behind(body, edge):
    own_rows = body.shape[0] - HALF_ROWS
    west = moved(edge, "lon", 1)[:, :HALF_COLS]
    whole = jnp.concatenate([west, body[:, HALF_COLS:]], 1)
    north = moved(whole[own_rows:], "lat", 1)
    return jnp.concatenate([north, whole[:own_rows]], 0)


def scatter_over(value, axis):
    return lax.psum_scatter(value, axis, scatter_dimension=0, tiled=True)


def local(latent, w_qkv, w_proj, w_fc1, w_fc2, w_head, target_bins, land_mask):
    width = latent.shape[2]
    lats, lons = lax.axis_size("lat"), lax.axis_size("lon")
    devices = lats * lons
    linked = lons == 8 and lats > 2 and width % (16 * devices) == 0
    weights = (w_qkv, w_proj, w_fc1, w_fc2, w_head)
    if linked:
        return tuple(device_step(latent, (), target_bins, land_mask, (), weights, lats, lons, True))
    marks = jnp.concatenate([target_bins, land_mask[:, :, None]], 2).astype(F32)
    marks = jnp.pad(marks, ((0, 0), (0, 0), (0, LANES - marks.shape[2])))
    body, edge, *grads = device_step(
        latent, edges_ahead(latent), target_bins, land_mask, edges_ahead(marks), weights, lats, lons, False
    )
    grad_latent = roll_behind(body, edge)

    def to_columns(grad):
        deep = grad.shape[0] // width
        parts = grad.reshape(devices, deep, width // devices, -1)
        return [parts[:, part].reshape(width, -1) for part in range(deep)]

    columns = [to_columns(grad) for grad in grads]
    joined = jnp.concatenate([part for group in columns for part in group], 1)
    summed = scatter_over(scatter_over(joined, "lat"), "lon").astype(F32)
    outs, start = [], 0
    for grad, group in zip(grads, columns):
        size = grad.shape[1]
        pieces = [summed[:, start + part * size : start + (part + 1) * size] for part in range(len(group))]
        outs.append(jnp.concatenate(pieces, 0))
        start += size * len(group)
    return (grad_latent, *outs)


def solution(mesh):
    grid = P("lat", "lon", None)
    spread = P(("lat", "lon"), None)
    return jax.shard_map(
        local,
        mesh=mesh,
        in_specs=(grid, P(), P(), P(), P(), P(), grid, P("lat", "lon")),
        out_specs=(grid, spread, spread, spread, spread, spread),
        check_vma=False,
    )
```
